256 devices in a mesh: mrow: 8 (over y, z_lo), pcol: 32 (over x, z_hi, core).
Axes of the slice: x: 4, y: 4, z: 8 (z_hi: 4, z_lo: 2; z = z_hi * 2 + z_lo), core: 2. Of those that a mesh axis runs over, the one named last changes fastest.
Arguments:
- snapshots: bfloat16 [7424, 8192], P('mrow', 'pcol'), may hold values from -16 to 16
- area_weight: float32 [8192], P('pcol'), may hold values from 0.2 to 1
Outputs:
- gram_tiles: float32 [8, 32, 215296], P('mrow', 'pcol')
The draws below stay inside these ranges and needn't reach their ends.
All inputs are finite; a program needn't handle non-finite values.
Results may differ from the reference program's by a relative error of at most 0.0003.
Values may be sent and summed in bfloat16 or wider, within the bound.
A program may use at most 64 MiB of HBM per device.

```python
import math
import jax
import jax.numpy as jnp
from jax import lax

MEMBERS = 7424
POINTS = 8192
N_MROW = 8
N_PCOL = 32


def draw_snapshots(key, part):
    base = jax.random.fold_in(key, 11)
    keys = jax.random.split(base, 6)
    mode_count = 96
    climate = 2.0 * jax.random.normal(keys[0], (1, POINTS), jnp.float32)
    ranks = jnp.arange(1, mode_count + 1).astype(jnp.float32)
    coeff = jax.random.normal(keys[1], (MEMBERS, mode_count), jnp.float32) * (ranks ** (-0.5))[None, :]
    freq = jax.random.randint(keys[2], (mode_count, 1), 1, 33).astype(jnp.float32)
    phase = jax.random.uniform(keys[3], (mode_count, 1), jnp.float32, 0.0, 2.0 * math.pi)
    position = (jnp.arange(POINTS).astype(jnp.float32) / POINTS)[None, :]
    shapes = math.sqrt(2.0) * jnp.cos(2.0 * math.pi * freq * position + phase)
    rough = jax.random.uniform(keys[4], (1, POINTS), jnp.float32, 0.6, 1.4)
    total_var = jnp.sum(1.0 / ranks)
    signal = jnp.dot(coeff, shapes, precision=lax.Precision.HIGHEST) / jnp.sqrt(total_var) * rough
    noise = jax.random.normal(keys[5], (MEMBERS, POINTS), jnp.float32)
    field = signal + 0.2 * noise
    return jnp.clip(climate + field, -16.0, 16.0).astype(jnp.bfloat16)


def levels(own_key, shape, cuts, low, top_value):
    loudness = 1.0
    for dim, shards_of in cuts:
        draws = jax.random.uniform(jax.random.fold_in(jax.random.fold_in(own_key, 6), dim), (shards_of,), jnp.float32, low / len(cuts), top_value / len(cuts))
        loudness = loudness * jnp.repeat(jnp.exp(draws), shape[dim] // shards_of).reshape((-1,) + (1,) * (len(shape) - 1 - dim))
    return loudness


def setup_inputs(seed: int = 0) -> dict:
    key_list = jax.random.split(jax.random.key(seed), 3)
    snapshots = draw_snapshots(jax.random.fold_in(key_list[2], 71), 0)
    area_weight = jnp.clip(jnp.exp(math.log(1.0) - 1.609438 * jax.random.uniform(key_list[1], (POINTS,), jnp.float32) ** levels(key_list[1], (POINTS,), ((0, 32),), -0.2, 0.2)), 0.2, 1.0)
    return {"snapshots": snapshots, "area_weight": area_weight}


def reference(snapshots, area_weight):
    ens_mean = lax.optimization_barrier(jnp.sum(snapshots.astype(jnp.float32), axis=0)) / MEMBERS
    anomaly = ((snapshots.astype(jnp.float32) - ens_mean[None, :]) * jnp.sqrt(area_weight)[None, :]).astype(jnp.bfloat16)
    wide = anomaly.astype(jnp.float32)
    gram = jnp.dot(wide, wide.T, precision=lax.Precision.HIGHEST, preferred_element_type=jnp.float32)
    gram = gram / (MEMBERS - 1)
    blocks = gram.reshape(N_MROW, MEMBERS // N_MROW, N_PCOL, MEMBERS // N_PCOL)
    blocks = jnp.transpose(blocks, (0, 2, 1, 3))
    return blocks.reshape(N_MROW, N_PCOL, MEMBERS // N_MROW * (MEMBERS // N_PCOL))
```

```python
import functools

import jax
import jax.numpy as jnp
from jax import lax
from jax.experimental import pallas as pl
from jax.experimental.pallas import tpu as pltpu
from jax.sharding import PartitionSpec as P

MEMBERS = 7424
MESH = pl.DeviceIdType.MESH


def device(x, y, p, lo, core):
    return (y * 2 + lo, x * 8 + p * 2 + core)


def kernel(
    x_ref, w_ref, out_ref, rows, cols, sums, part, peer,
    row_sem, col_sem, sum_sem, peer_sem, send_sem,
):
    half = x_ref.shape[0] // 2
    tile = half // 2
    me_row, me_col = lax.axis_index("mrow"), lax.axis_index("pcol")
    y, lo = me_row // 2, me_row % 2
    x, p, core = me_col // 8, (me_col // 2) % 4, me_col % 2
    hi, h = p // 2, p % 2

    xp, xm, x2 = (x + 1) % 4, (x + 3) % 4, (x + 2) % 4
    pp, pm, p2 = (p + 1) % 4, (p + 3) % 4, (p + 2) % 4
    yp, ym, y2 = (y + 1) % 4, (y + 3) % 4, (y + 2) % 4
    x_plus, x_minus = device(xp, y, p, lo, core), device(xm, y, p, lo, core)
    z_plus, z_minus = device(x, y, pp, lo, core), device(x, y, pm, lo, core)
    y_plus, y_minus = device(x, yp, p, lo, core), device(x, ym, p, lo, core)
    z_pair = device(x, y, p, 1 - lo, core)
    twin = device(x, y, p, lo, 1 - core)

    turn_lo = ((p + 1) // 2) % 2
    turned = [device(y, x, 2 * lo + s, turn_lo, core) for s in range(2)]
    turn_self = [(x == y) & (2 * lo + s == p) & (turn_lo == lo) for s in range(2)]
    first_p = [lo, 3 - lo]
    turn_from = [device(y, x, q, hi, core) for q in first_p]
    from_self = [(x == y) & (q == p) & (hi == lo) for q in first_p]
    others = [((me_row + d) % 8, me_col) for d in range(1, 8)]

    barrier = pltpu.get_barrier_semaphore()

    def greet(dev):
        pl.semaphore_signal(barrier, inc=1, device_id=dev, device_id_type=MESH)

    for dev in (x_plus, x_minus, z_plus, z_minus, y_plus, y_minus, z_pair, twin, *others):
        greet(dev)
    for s in range(2):
        @pl.when(jnp.logical_not(from_self[s]))
        def _():
            greet(turn_from[s])

    sums[pl.ds(me_row, 1)] = jnp.sum(x_ref[...].astype(jnp.float32), axis=0, keepdims=True)[None]
    stay = jnp.where(turn_self[0], 1, 0) + jnp.where(turn_self[1], 1, 0)
    pl.semaphore_wait(barrier, 17 - stay)

    sends = []

    def send(src, dst, recv_sem, dev):
        n = len(sends)
        copy = pltpu.make_async_remote_copy(
            src_ref=src, dst_ref=dst, send_sem=send_sem.at[n], recv_sem=recv_sem,
            device_id=dev, device_id_type=MESH,
        )
        copy.start()
        sends.append(copy)

    def arrived(ref, recv_sem):
        pltpu.make_async_remote_copy(
            src_ref=ref, dst_ref=ref, send_sem=send_sem.at[0], recv_sem=recv_sem,
            device_id=twin, device_id_type=MESH,
        ).wait_recv()

    for d in range(7):
        slot = sums.at[me_row]
        send(slot, slot, sum_sem.at[me_row], others[d])
    for d in range(1, 8):
        q = (me_row + d) % 8
        arrived(sums.at[q], sum_sem.at[q])
    mean = jnp.sum(sums[...], axis=0) / MEMBERS
    own = x * 4 + p
    rows[pl.ds(own, 1)] = (
        ((x_ref[...].astype(jnp.float32) - mean) * jnp.sqrt(w_ref[...])).astype(jnp.bfloat16)
    )[None]

    def row_half(i, s):
        return rows.at[i, pl.ds(s * half, half)]

    def send_row(i, s, dev):
        send(row_half(i, s), row_half(i, s), row_sem.at[i, s], dev)

    def row_arrived(i, s):
        arrived(row_half(i, s), row_sem.at[i, s])

    def send_col(i, dev):
        send(cols.at[i], cols.at[i], col_sem.at[i], dev)

    def col_arrived(i):
        arrived(cols.at[i], col_sem.at[i])

    turns = []
    for s in range(2):
        n = 64 + s
        copy = pltpu.make_async_remote_copy(
            src_ref=row_half(own, s), dst_ref=cols.at[own], send_sem=send_sem.at[n],
            recv_sem=col_sem.at[own], device_id=turned[s], device_id_type=MESH,
        )
        turns.append(copy)

        @pl.when(jnp.logical_not(turn_self[s]))
        def _():
            copy.start()

        @pl.when(turn_self[s])
        def _():
            cols[pl.ds(own, 1)] = rows[pl.ds(own, 1), s * half:(s + 1) * half]

    def x_sends(i, s):
        send_row(i, s, x_plus)
        send_row(i, s, x_minus)

    def x_forward(q):
        i, j = xm * 4 + q, xp * 4 + q
        row_arrived(i, 0)
        send_row(i, 0, x_plus)
        row_arrived(j, 1)
        send_row(j, 1, x_minus)

    send_row(own, 0, x_plus)
    send_row(own, 1, x_minus)
    send_row(own, 0, z_plus)
    send_row(own, 1, z_minus)
    send_row(own, 1, x_plus)
    send_row(own, 0, x_minus)
    send_row(own, 1, z_plus)
    send_row(own, 0, z_minus)

    x_forward(p)

    firsts = [y * 4 + q for q in first_p]
    for s in range(2):
        @pl.when(jnp.logical_not(from_self[s]))
        def _():
            col_arrived(firsts[s])
    for s in range(2):
        send_col(firsts[s], z_pair)
        send_col(firsts[s], y_plus)
        send_col(firsts[s], y_minus)

    i, j = x * 4 + pm, x * 4 + pp
    row_arrived(i, 0)
    send_row(i, 0, z_plus)
    x_sends(i, 0)
    row_arrived(j, 1)
    send_row(j, 1, z_minus)
    x_sends(j, 1)
    row_arrived(i, 1)
    x_sends(i, 1)
    row_arrived(j, 0)
    x_sends(j, 0)

    seconds = [y * 4 + q for q in (1 - lo, 2 + lo)]
    for s in range(2):
        col_arrived(seconds[s])
        send_col(seconds[s], y_plus)
        send_col(seconds[s], y_minus)

    col_arrived(ym * 4 + first_p[0])
    send_col(ym * 4 + first_p[0], y_plus)
    col_arrived(yp * 4 + first_p[1])
    send_col(yp * 4 + first_p[1], y_minus)

    x_forward(pm)
    x_forward(pp)

    k = x * 4 + p2
    row_arrived(k, 0)
    x_sends(k, 0)
    row_arrived(k, 1)
    x_sends(k, 1)

    col_arrived(ym * 4 + 1 - lo)
    send_col(ym * 4 + 1 - lo, y_plus)
    col_arrived(yp * 4 + 2 + lo)
    send_col(yp * 4 + 2 + lo, y_minus)

    x_forward(p2)

    for i in (ym * 4 + first_p[1], yp * 4 + first_p[0], ym * 4 + 2 + lo, yp * 4 + 1 - lo):
        col_arrived(i)
    for q in range(4):
        col_arrived(y2 * 4 + q)

    contract = (((1,), (1,)), ((), ()))

    def add(i, first):
        block = rows[i]
        column = cols[i]
        for c in range(2):
            term = lax.dot_general(
                block, column[c * tile:(c + 1) * tile], contract, preferred_element_type=jnp.float32
            )
            if first:
                part[c] = term
            else:
                part[c] += term

    add(own, True)
    for q in (pm, pp, p2):
        add(x * 4 + q, False)

    def per_p(step, _):
        q = (p + jnp.where(step == 0, 0, jnp.where(step == 1, 3, jnp.where(step == 2, 1, 2)))) % 4
        row_arrived(xm * 4 + q, 1)
        add(xm * 4 + q, False)
        row_arrived(xp * 4 + q, 0)
        add(xp * 4 + q, False)
        row_arrived(x2 * 4 + q, 0)
        row_arrived(x2 * 4 + q, 1)
        add(x2 * 4 + q, False)
        return 0

    lax.fori_loop(0, 4, per_p, 0)

    send(part.at[1 - core], peer, peer_sem, twin)
    arrived(peer, peer_sem)
    out_ref[...] = (part[core] + peer[...]) / (MEMBERS - 1)

    for copy in sends:
        copy.wait_send()
    for s in range(2):
        @pl.when(jnp.logical_not(turn_self[s]))
        def _():
            turns[s].wait_send()


def local(snapshots, area_weight):
    members, points = snapshots.shape
    tile = members // 4
    vmem = pl.BlockSpec(memory_space=pltpu.VMEM)
    gram = pl.pallas_call(
        kernel,
        out_shape=jax.ShapeDtypeStruct((members, tile), jnp.float32),
        in_specs=[vmem, vmem],
        out_specs=vmem,
        scratch_shapes=[
            pltpu.VMEM((16, members, points), jnp.bfloat16),
            pltpu.VMEM((16, members // 2, points), jnp.bfloat16),
            pltpu.VMEM((8, 1, points), jnp.float32),
            pltpu.VMEM((2, members, tile), jnp.float32),
            pltpu.VMEM((members, tile), jnp.float32),
            pltpu.SemaphoreType.DMA((16, 2)),
            pltpu.SemaphoreType.DMA((16,)),
            pltpu.SemaphoreType.DMA((8,)),
            pltpu.SemaphoreType.DMA,
            pltpu.SemaphoreType.DMA((66,)),
        ],
        compiler_params=pltpu.CompilerParams(collective_id=0, has_side_effects=True),
    )(snapshots, area_weight.reshape(1, points))
    return gram.reshape(1, 1, members * tile)


def solution(mesh):
    return jax.shard_map(
        local,
        mesh=mesh,
        in_specs=(P("mrow", "pcol"), P("pcol")),
        out_specs=P("mrow", "pcol", None),
        check_vma=False,
    )
```

```python
import jax
import jax.numpy as jnp
from jax import lax
from jax.experimental import pallas as pl
from jax.experimental.pallas import tpu as pltpu
from jax.sharding import PartitionSpec as P

MEMBERS = 7424
MESH = pl.DeviceIdType.MESH
SENDS = 80


def device(x, y, p, lo, core):
    return (y * 2 + lo, x * 8 + p * 2 + core)


def kernel(
    x_ref, w_ref, out_ref, rows, cols, anom, canom, passing, sums, ysums, table, part, peer,
    row_sem, col_sem, pass_sem, sum_sem, ysum_sem, ztab_sem, xtab_sem, peer_sem, send_sem,
):
    half = x_ref.shape[0] // 2
    tile = half // 2
    me_row, me_col = lax.axis_index("mrow"), lax.axis_index("pcol")
    y, lo = me_row // 2, me_row % 2
    x, p, core = me_col // 8, (me_col // 2) % 4, me_col % 2
    hi = p // 2

    xp, xm, x2 = (x + 1) % 4, (x + 3) % 4, (x + 2) % 4
    pp, pm, p2 = (p + 1) % 4, (p + 3) % 4, (p + 2) % 4
    yp, ym, y2 = (y + 1) % 4, (y + 3) % 4, (y + 2) % 4
    x_plus, x_minus, x_far = (device(v, y, p, lo, core) for v in (xp, xm, x2))
    z_plus, z_minus, z_far = (device(x, y, v, lo, core) for v in (pp, pm, p2))
    y_plus, y_minus, y_far = (device(x, v, p, lo, core) for v in (yp, ym, y2))
    z_pair = device(x, y, p, 1 - lo, core)
    twin = device(x, y, p, lo, 1 - core)
    own = x * 4 + p
    diagonal = x == y

    def origin(v):
        return (v + 2 * ((x + v + 1) % 2)) % 4


    turn_lo = ((p + 1) // 2) % 2
    turned = [device(x, y, 2 * lo + s, turn_lo, core) for s in range(2)]
    stays = [(2 * lo + s == p) & (turn_lo == lo) for s in range(2)]
    moves = [jnp.logical_not(v) for v in stays]
    first_p = [lo, 3 - lo]
    second_p = [1 - lo, 2 + lo]
    turn_from = [device(x, y, q, hi, core) for q in first_p]
    from_here = [(q == p) & (hi == lo) for q in first_p]

    barrier = pltpu.get_barrier_semaphore()

    def greet(dev):
        pl.semaphore_signal(barrier, inc=1, device_id=dev, device_id_type=MESH)

    for dev in (x_plus, x_minus, x_far, z_plus, z_minus, z_far, y_plus, y_minus, y_far, z_pair, twin):
        greet(dev)
    for s in range(2):
        @pl.when(jnp.logical_not(from_here[s]))
        def _():
            greet(turn_from[s])

    sums[pl.ds(0, 1)] = jnp.sum(x_ref[...].astype(jnp.float32), axis=0, keepdims=True)[None]
    pl.semaphore_wait(barrier, 13 - jnp.where(stays[0], 1, 0) - jnp.where(stays[1], 1, 0))

    sends = []
    count = [0]

    def copy_to(src, dst, recv_sem, dev, n):
        return pltpu.make_async_remote_copy(
            src_ref=src, dst_ref=dst, send_sem=send_sem.at[n], recv_sem=recv_sem,
            device_id=dev, device_id_type=MESH,
        )

    def new_sem():
        count[0] += 1
        return count[0] - 1

    def send(src, dst, recv_sem, dev):
        copy = copy_to(src, dst, recv_sem, dev, new_sem())
        copy.start()
        sends.append(copy)

    def arrived(ref, recv_sem):
        copy_to(ref, ref, recv_sem, twin, 0).wait_recv()

    def row_half(i, s):
        return rows.at[i, pl.ds(s * half, half)]

    def own_half(s):
        return x_ref.at[pl.ds(s * half, half)]

    def send_own(s, dev):
        send(own_half(s), row_half(own, s), row_sem.at[own, s], dev)

    def send_row(i, s, dev):
        send(row_half(i, s), row_half(i, s), row_sem.at[i, s], dev)

    def row_arrived(i, s):
        arrived(row_half(i, s), row_sem.at[i, s])

    def send_col(i, dev):
        send(cols.at[i], cols.at[i], col_sem.at[i], dev)

    def col_arrived(i):
        arrived(cols.at[i], col_sem.at[i])

    def x_sends(i, s):
        send_row(i, s, x_plus)
        send_row(i, s, x_minus)

    def x_forward(q):
        i, j = xm * 4 + q, xp * 4 + q
        row_arrived(i, 0)
        send_row(i, 0, x_plus)
        row_arrived(j, 1)
        send_row(j, 1, x_minus)

    pushes = []

    def push(src, i, s, dev):
        n = new_sem()

        @pl.when(diagonal & stays[s])
        def _():
            copy_to(src, cols.at[i], col_sem.at[i], dev, n).start()

        @pl.when(diagonal & moves[s])
        def _():
            copy_to(src, passing.at[s], pass_sem.at[s], dev, n).start()

        pushes.append((src, n))

    def push_row(v, s, dev):
        push(row_half(v * 4 + p, s), v * 4 + p, s, dev)

    turns = []

    def turn_on(s):
        n = new_sem()
        i = origin(y) * 4 + p

        @pl.when(diagonal & moves[s])
        def _():
            copy_to(row_half(x2 * 4 + p, s), cols.at[i], col_sem.at[i], turned[s], n).start()

        @pl.when(diagonal & stays[s])
        def _():
            cols[pl.ds(i, 1)] = rows[pl.ds(x2 * 4 + p, 1), s * half:(s + 1) * half]

        @pl.when(jnp.logical_not(diagonal) & moves[s])
        def _():
            arrived(passing.at[s], pass_sem.at[s])
            copy_to(passing.at[s], cols.at[i], col_sem.at[i], turned[s], n).start()

        turns.append((s, n))

    def to_anomaly(block, i):
        entry = table[i]
        return ((block.astype(jnp.float32) - entry[0:1]) * entry[1:2]).astype(jnp.bfloat16)

    def row_anomaly(i):
        anom[pl.ds(i, 1)] = to_anomaly(rows[i], i)[None]

    def col_anomaly(i):
        canom[pl.ds(i, 1)] = to_anomaly(cols[i], i)[None]

    contract = (((1,), (1,)), ((), ()))

    def add(i):
        block = anom[i]
        column = canom[i]
        for c in range(2):
            part[c] += lax.dot_general(
                block, column[c * tile:(c + 1) * tile], contract, preferred_element_type=jnp.float32
            )

    def nth(step):
        return (p + jnp.where(step == 0, 3, jnp.where(step == 1, 1, 2))) % 4

    def start():
        send(sums.at[0], sums.at[1], sum_sem, z_pair)
        send_own(0, x_plus)
        send_own(1, x_minus)
        send_own(0, z_plus)
        send_own(1, z_minus)
        push(own_half(0), own, 0, y_far)
        push(own_half(1), own, 1, y_far)

    def means():
        arrived(sums.at[1], sum_sem)
        ysums[pl.ds(y, 1)] = (sums[0] + sums[1])[None]
        for dev in (y_plus, y_minus, y_far):
            send(ysums.at[y], ysums.at[y], ysum_sem.at[y], dev)
        send_own(1, x_plus)
        send_own(0, x_minus)
        for v in (yp, ym, y2):
            arrived(ysums.at[v], ysum_sem.at[v])
        mean = jnp.sum(ysums[...], axis=0) / MEMBERS
        table[pl.ds(own, 1)] = jnp.concatenate([mean, jnp.sqrt(w_ref[...])], axis=0)[None]
        for dev in (z_plus, z_minus, z_far):
            send(table.at[own], table.at[own], ztab_sem.at[p], dev)
        send_own(1, z_plus)
        send_own(0, z_minus)

    def near_push():
        push_row(xm, 0, y_minus)
        push_row(xp, 1, y_plus)

    def z_first():
        i, j = x * 4 + pm, x * 4 + pp
        row_arrived(i, 0)
        x_sends(i, 0)
        row_arrived(j, 1)
        x_sends(j, 1)

    def z_fwd():
        send_row(x * 4 + pm, 0, z_plus)
        send_row(x * 4 + pp, 1, z_minus)

    def near_push2():
        row_arrived(xm * 4 + p, 1)
        push_row(xm, 1, y_minus)
        row_arrived(xp * 4 + p, 0)
        push_row(xp, 0, y_plus)

    def tables():
        for q in (pp, pm, p2):
            arrived(table.at[x * 4 + q], ztab_sem.at[q])
        group = table.at[pl.ds(x * 4, 4)]
        for dev in (x_plus, x_minus, x_far):
            send(group, group, xtab_sem.at[x], dev)

    def far_rows():
        row_arrived(x2 * 4 + p, 0)
        row_arrived(x2 * 4 + p, 1)

    def z_second():
        i, j = x * 4 + pm, x * 4 + pp
        row_arrived(i, 1)
        x_sends(i, 1)
        row_arrived(j, 0)
        x_sends(j, 0)

    def turn_all():
        turn_on(0)
        turn_on(1)

    def x_fwd0():
        x_forward(p)

    def x_fwd1():
        x_forward(pm)
        x_forward(pp)

    def x_fwd2():
        x_forward(p2)

    def firsts():
        for s in range(2):
            i = origin(y) * 4 + first_p[s]

            @pl.when(jnp.logical_not(from_here[s] & diagonal))
            def _():
                col_arrived(i)

            send_col(i, z_pair)
            send_col(i, y_plus)
            send_col(i, y_minus)

    def z_far_rows():
        k = x * 4 + p2
        for s in range(2):
            row_arrived(k, s)
            x_sends(k, s)

    def seconds():
        for q in second_p:
            col_arrived(origin(y) * 4 + q)
            send_col(origin(y) * 4 + q, y_plus)
            send_col(origin(y) * 4 + q, y_minus)

    def tables2():
        for v in (xp, xm, x2):
            arrived(table.at[pl.ds(v * 4, 4)], xtab_sem.at[v])

    def y_fwd(pair):
        a, b = pair
        col_arrived(origin(ym) * 4 + a)
        send_col(origin(ym) * 4 + a, y_plus)
        col_arrived(origin(yp) * 4 + b)
        send_col(origin(yp) * 4 + b, y_minus)

    def y_fwd1():
        y_fwd(first_p)

    def y_fwd2():
        y_fwd(second_p)

    def near_anomalies():
        anom[pl.ds(own, 1)] = to_anomaly(x_ref[...], own)[None]
        part[...] = jnp.zeros_like(part)
        for v in (xm, xp, x2):
            row_anomaly(v * 4 + p)

    def rest(step, _):
        q = nth(step)
        row_arrived(xm * 4 + q, 1)
        row_arrived(xp * 4 + q, 0)
        row_arrived(x2 * 4 + q, 0)
        row_arrived(x2 * 4 + q, 1)
        for v in (x, xm, xp, x2):
            row_anomaly(v * 4 + q)
        return 0

    def rest2():
        lax.fori_loop(0, 2, rest, 0)

    def rest_cols():
        for a, b in (first_p, second_p):
            col_arrived(origin(ym) * 4 + b)
            col_arrived(origin(yp) * 4 + a)
        for q in range(4):
            col_arrived(origin(y2) * 4 + q)

    def compute():
        def col_all(i, _):
            col_anomaly(i)
            return 0

        lax.fori_loop(0, 16, col_all, 0)

        def products(n, _):
            q = (p + 3 + n // 4) % 4
            add((n % 4) * 4 + q)
            return 0

        lax.fori_loop(0, 12, products, 0)
        lax.fori_loop(2, 3, rest, 0)
        lax.fori_loop(12, 16, products, 0)

    for step in (
        start, means, x_fwd0, near_push, z_first, near_push2, tables, far_rows, turn_all, z_second, z_fwd,
        firsts, x_fwd1, z_far_rows, seconds, tables2, near_anomalies, y_fwd1, y_fwd2, x_fwd2, rest2,
        rest_cols, compute,
    ):
        step()

    send(part.at[1 - core], peer, peer_sem, twin)
    arrived(peer, peer_sem)
    out_ref[...] = (part[core] + peer[...]) / (MEMBERS - 1)

    for copy in sends:
        copy.wait_send()
    for src, n in pushes:
        @pl.when(diagonal)
        def _():
            copy_to(src, src, pass_sem.at[0], twin, n).wait_send()
    for s, n in turns:
        @pl.when(moves[s])
        def _():
            copy_to(passing.at[s], passing.at[s], pass_sem.at[0], twin, n).wait_send()


def local(snapshots, area_weight):
    members, points = snapshots.shape
    tile = members // 4
    vmem = pl.BlockSpec(memory_space=pltpu.VMEM)
    dma = pltpu.SemaphoreType.DMA
    gram = pl.pallas_call(
        kernel,
        out_shape=jax.ShapeDtypeStruct((members, tile), jnp.float32),
        in_specs=[vmem, vmem],
        out_specs=vmem,
        scratch_shapes=[
            pltpu.VMEM((16, members, points), jnp.bfloat16),
            pltpu.VMEM((16, members // 2, points), jnp.bfloat16),
            pltpu.VMEM((16, members, points), jnp.bfloat16),
            pltpu.VMEM((16, members // 2, points), jnp.bfloat16),
            pltpu.VMEM((2, members // 2, points), jnp.bfloat16),
            pltpu.VMEM((2, 1, points), jnp.float32),
            pltpu.VMEM((4, 1, points), jnp.float32),
            pltpu.VMEM((16, 2, points), jnp.float32),
            pltpu.VMEM((2, members, tile), jnp.float32),
            pltpu.VMEM((members, tile), jnp.float32),
            dma((16, 2)),
            dma((16,)),
            dma((2,)),
            dma,
            dma((4,)),
            dma((4,)),
            dma((4,)),
            dma,
            dma((SENDS,)),
        ],
        compiler_params=pltpu.CompilerParams(collective_id=0, has_side_effects=True),
    )(snapshots, area_weight.reshape(1, points))
    return gram.reshape(1, 1, members * tile)


def solution(mesh):
    return jax.shard_map(
        local,
        mesh=mesh,
        in_specs=(P("mrow", "pcol"), P("pcol")),
        out_specs=P("mrow", "pcol", None),
        check_vma=False,
    )
```

```python
import jax
import jax.numpy as jnp
from jax import lax
from jax.experimental import pallas as pl
from jax.experimental.pallas import tpu as pltpu
from jax.sharding import PartitionSpec as P

MEMBERS = 7424
MESH = pl.DeviceIdType.MESH
SENDS = 80


def device(x, y, p, lo, core):
    return (y * 2 + lo, x * 8 + p * 2 + core)


def kernel(
    x_ref, w_ref, out_ref, rows, cols, passing, sums, ysums, table, part, peer,
    row_sem, col_sem, pass_sem, sum_sem, ysum_sem, ztab_sem, xtab_sem, peer_sem, send_sem,
):
    half = x_ref.shape[0] // 2
    tile = half // 2
    me_row, me_col = lax.axis_index("mrow"), lax.axis_index("pcol")
    y, lo = me_row // 2, me_row % 2
    x, p, core = me_col // 8, (me_col // 2) % 4, me_col % 2
    hi = p // 2

    xp, xm, x2 = (x + 1) % 4, (x + 3) % 4, (x + 2) % 4
    pp, pm, p2 = (p + 1) % 4, (p + 3) % 4, (p + 2) % 4
    yp, ym, y2 = (y + 1) % 4, (y + 3) % 4, (y + 2) % 4
    x_plus, x_minus, x_far = (device(v, y, p, lo, core) for v in (xp, xm, x2))
    z_plus, z_minus, z_far = (device(x, y, v, lo, core) for v in (pp, pm, p2))
    y_plus, y_minus, y_far = (device(x, v, p, lo, core) for v in (yp, ym, y2))
    z_pair = device(x, y, p, 1 - lo, core)
    twin = device(x, y, p, lo, 1 - core)
    own = x * 4 + p
    diagonal = x == y

    def origin(v):
        return (v + 2 * ((x + v + 1) % 2)) % 4


    turn_lo = [((lo + s - p) % 4) // 2 for s in range(2)]
    turned = [device(x, y, 2 * lo + s, turn_lo[s], core) for s in range(2)]
    stays = [2 * lo + s == p for s in range(2)]
    moves = [jnp.logical_not(v) for v in stays]
    first_p = [(p - hi - 3 * lo) % 4, (p - hi - 1 - lo) % 4]
    second_p = [(p - hi - 3 * (1 - lo)) % 4, (p - hi - 2 + lo) % 4]
    turn_from = [device(x, y, q, hi, core) for q in first_p]
    from_here = [(q == p) & (hi == lo) for q in first_p]

    barrier = pltpu.get_barrier_semaphore()

    def greet(dev):
        pl.semaphore_signal(barrier, inc=1, device_id=dev, device_id_type=MESH)

    for dev in (x_plus, x_minus, x_far, z_plus, z_minus, z_far, y_plus, y_minus, y_far, z_pair, twin):
        greet(dev)
    for s in range(2):
        @pl.when(jnp.logical_not(from_here[s]))
        def _():
            greet(turn_from[s])

    sums[pl.ds(0, 1)] = jnp.sum(x_ref[...].astype(jnp.float32), axis=0, keepdims=True)[None]
    pl.semaphore_wait(barrier, 13 - jnp.where(hi == lo, 1, 0))

    sends = []
    count = [0]

    def copy_to(src, dst, recv_sem, dev, n):
        return pltpu.make_async_remote_copy(
            src_ref=src, dst_ref=dst, send_sem=send_sem.at[n], recv_sem=recv_sem,
            device_id=dev, device_id_type=MESH,
        )

    def new_sem():
        count[0] += 1
        return count[0] - 1

    def send(src, dst, recv_sem, dev):
        copy = copy_to(src, dst, recv_sem, dev, new_sem())
        copy.start()
        sends.append(copy)

    def arrived(ref, recv_sem):
        copy_to(ref, ref, recv_sem, twin, 0).wait_recv()

    def row_half(i, s):
        return rows.at[i, pl.ds(s * half, half)]

    def own_half(s):
        return x_ref.at[pl.ds(s * half, half)]

    def send_own(s, dev):
        send(own_half(s), row_half(own, s), row_sem.at[own, s], dev)

    def send_row(i, s, dev):
        send(row_half(i, s), row_half(i, s), row_sem.at[i, s], dev)

    def row_arrived(i, s):
        arrived(row_half(i, s), row_sem.at[i, s])

    def send_col(i, dev):
        send(cols.at[i], cols.at[i], col_sem.at[i], dev)

    def col_arrived(i):
        arrived(cols.at[i], col_sem.at[i])

    def x_sends(i, s):
        send_row(i, s, x_plus)
        send_row(i, s, x_minus)

    def x_forward(q):
        i, j = xm * 4 + q, xp * 4 + q
        row_arrived(i, 0)
        send_row(i, 0, x_plus)
        row_arrived(j, 1)
        send_row(j, 1, x_minus)

    pushes = []

    def push(src, i, s, dev):
        n = new_sem()

        @pl.when(diagonal & stays[s])
        def _():
            copy_to(src, cols.at[i], col_sem.at[i], dev, n).start()

        @pl.when(diagonal & moves[s])
        def _():
            copy_to(src, passing.at[s], pass_sem.at[s], dev, n).start()

        pushes.append((src, n))

    def push_row(v, s, dev):
        push(row_half(v * 4 + p, s), v * 4 + p, s, dev)

    turns = []

    def turn_on(s):
        n = new_sem()
        i = origin(y) * 4 + p

        @pl.when(diagonal & moves[s])
        def _():
            copy_to(row_half(x2 * 4 + p, s), cols.at[i], col_sem.at[i], turned[s], n).start()

        @pl.when(diagonal & stays[s])
        def _():
            cols[pl.ds(i, 1)] = rows[pl.ds(x2 * 4 + p, 1), s * half:(s + 1) * half]

        @pl.when(jnp.logical_not(diagonal) & moves[s])
        def _():
            arrived(passing.at[s], pass_sem.at[s])
            copy_to(passing.at[s], cols.at[i], col_sem.at[i], turned[s], n).start()

        turns.append((s, n))

    def to_anomaly(block, i):
        entry = table[i]
        return ((block.astype(jnp.float32) - entry[0:1]) * entry[1:2]).astype(jnp.bfloat16)

    contract = (((1,), (1,)), ((), ()))

    def nth(n, values):
        value = values[0]
        for k in range(1, len(values)):
            value = jnp.where(n == k, values[k], value)
        return value

    def start():
        send(sums.at[0], sums.at[1], sum_sem, z_pair)
        send_own(0, x_plus)
        send_own(1, x_minus)
        send_own(0, z_plus)
        send_own(1, z_minus)
        send_own(1, x_plus)
        send_own(0, x_minus)

    def pair_sums():
        arrived(sums.at[1], sum_sem)
        ysums[pl.ds(y, 1)] = (sums[0] + sums[1])[None]
        for dev in (y_plus, y_minus, y_far):
            send(ysums.at[y], ysums.at[y], ysum_sem.at[y], dev)
        push(own_half(0), own, 0, y_far)
        push(own_half(1), own, 1, y_far)

    def means():
        for v in (yp, ym, y2):
            arrived(ysums.at[v], ysum_sem.at[v])
        mean = jnp.sum(ysums[...], axis=0) / MEMBERS
        table[pl.ds(own, 1)] = jnp.concatenate([mean, jnp.sqrt(w_ref[...])], axis=0)[None]
        for dev in (z_plus, z_minus, z_far):
            send(table.at[own], table.at[own], ztab_sem.at[p], dev)
        send_own(1, z_plus)
        send_own(0, z_minus)

    def near_push():
        push_row(xm, 0, y_minus)
        push_row(xp, 1, y_plus)

    def z_first():
        i, j = x * 4 + pm, x * 4 + pp
        row_arrived(i, 0)
        x_sends(i, 0)
        row_arrived(j, 1)
        x_sends(j, 1)

    def z_fwd():
        send_row(x * 4 + pm, 0, z_plus)
        send_row(x * 4 + pp, 1, z_minus)

    def near_push2():
        row_arrived(xm * 4 + p, 1)
        push_row(xm, 1, y_minus)
        row_arrived(xp * 4 + p, 0)
        push_row(xp, 0, y_plus)

    def tables():
        for q in (pp, pm, p2):
            arrived(table.at[x * 4 + q], ztab_sem.at[q])
        group = table.at[pl.ds(x * 4, 4)]
        for dev in (x_plus, x_minus, x_far):
            send(group, group, xtab_sem.at[x], dev)

    def far_rows():
        row_arrived(x2 * 4 + p, 0)
        row_arrived(x2 * 4 + p, 1)

    def z_second():
        i, j = x * 4 + pm, x * 4 + pp
        row_arrived(i, 1)
        x_sends(i, 1)
        row_arrived(j, 0)
        x_sends(j, 0)

    def turn0():
        turn_on(0)

    def turn1():
        turn_on(1)

    def x_fwd0():
        x_forward(p)

    def x_fwd1():
        x_forward(pm)
        x_forward(pp)

    def x_fwd2():
        x_forward(p2)

    def first(s):
        i = origin(y) * 4 + first_p[s]

        @pl.when(jnp.logical_not(from_here[s] & diagonal))
        def _():
            col_arrived(i)

        send_col(i, z_pair)
        send_col(i, y_plus)
        send_col(i, y_minus)

    def first0():
        first(0)

    def first1():
        first(1)

    def z_far_rows():
        k = x * 4 + p2
        for s in range(2):
            row_arrived(k, s)
            x_sends(k, s)

    def second(s):
        i = origin(y) * 4 + second_p[s]
        col_arrived(i)
        send_col(i, y_plus)
        send_col(i, y_minus)

    def second0():
        second(0)

    def second1():
        second(1)

    def tables2():
        for v in (xp, xm, x2):
            arrived(table.at[pl.ds(v * 4, 4)], xtab_sem.at[v])

    def y_fwd():
        i, j = origin(ym) * 4 + first_p[0], origin(yp) * 4 + first_p[1]
        col_arrived(i)
        send_col(i, y_plus)
        col_arrived(j)
        send_col(j, y_minus)

    def far_pass():
        for q in first_p:
            col_arrived(origin(y2) * 4 + q)
            send_col(origin(y2) * 4 + q, z_pair)

    def rows_rest(q):
        row_arrived(xm * 4 + q, 1)
        row_arrived(xp * 4 + q, 0)
        row_arrived(x2 * 4 + q, 0)
        row_arrived(x2 * 4 + q, 1)

    f0, f1 = first_p
    s0, s1 = second_p
    order = (
        (y, f0), (y, f1), (y, s0), (y, s1),
        (ym, f0), (yp, f1), (ym, f1), (yp, f0), (y2, f0), (y2, f1),
        (ym, s0), (yp, s0), (ym, s1), (yp, s1), (y2, s0), (y2, s1),
    )

    def products(first, last, wanted, wait):
        def product(n, _):
            i = nth(n, [origin(v) * 4 + q for v, q in order[first:last]])
            if wait:
                @pl.when((n == 2) | (n == 3) if first == 4 else n >= 0)
                def _():
                    col_arrived(i)

            @pl.when(wanted(i % 4))
            def _():
                block = to_anomaly(rows[i], i)
                column = to_anomaly(cols[i], i)
                for c in range(2):
                    part[c] += lax.dot_general(
                        block, column[c * tile:(c + 1) * tile], contract,
                        preferred_element_type=jnp.float32,
                    )
            return 0

        lax.fori_loop(0, last - first, product, 0)

    def near(q):
        return q != p2

    def far(q):
        return q == p2

    def prod_a():
        rows_rest(pm)
        rows_rest(pp)
        rows[pl.ds(own, 1)] = x_ref[...][None]
        part[...] = jnp.zeros_like(part)
        products(0, 4, near, False)

    def prod_b():
        products(4, 10, near, True)

    def prod_c():
        products(10, 16, near, True)

    def prod_d():
        rows_rest(p2)
        products(0, 16, far, False)

    for step in (
        start, pair_sums, means, x_fwd0, near_push, near_push2, z_first, far_rows, turn0, turn1, tables, z_second, z_fwd, first0, first1, x_fwd1, y_fwd, z_far_rows, second0, second1, tables2, far_pass, prod_a, x_fwd2, prod_b, prod_c, prod_d,
    ):
        step()

    send(part.at[1 - core], peer, peer_sem, twin)
    arrived(peer, peer_sem)
    out_ref[...] = (part[core] + peer[...]) / (MEMBERS - 1)

    for copy in sends:
        copy.wait_send()
    for src, n in pushes:
        @pl.when(diagonal)
        def _():
            copy_to(src, src, pass_sem.at[0], twin, n).wait_send()
    for s, n in turns:
        @pl.when(moves[s])
        def _():
            copy_to(passing.at[s], passing.at[s], pass_sem.at[0], twin, n).wait_send()


def local(snapshots, area_weight):
    members, points = snapshots.shape
    tile = members // 4
    vmem = pl.BlockSpec(memory_space=pltpu.VMEM)
    dma = pltpu.SemaphoreType.DMA
    gram = pl.pallas_call(
        kernel,
        out_shape=jax.ShapeDtypeStruct((members, tile), jnp.float32),
        in_specs=[vmem, vmem],
        out_specs=vmem,
        scratch_shapes=[
            pltpu.VMEM((16, members, points), jnp.bfloat16),
            pltpu.VMEM((16, members // 2, points), jnp.bfloat16),
            pltpu.VMEM((2, members // 2, points), jnp.bfloat16),
            pltpu.VMEM((2, 1, points), jnp.float32),
            pltpu.VMEM((4, 1, points), jnp.float32),
            pltpu.VMEM((16, 2, points), jnp.float32),
            pltpu.VMEM((2, members, tile), jnp.float32),
            pltpu.VMEM((members, tile), jnp.float32),
            dma((16, 2)),
            dma((16,)),
            dma((2,)),
            dma,
            dma((4,)),
            dma((4,)),
            dma((4,)),
            dma,
            dma((SENDS,)),
        ],
        compiler_params=pltpu.CompilerParams(collective_id=0, has_side_effects=True),
    )(snapshots, area_weight.reshape(1, points))
    return gram.reshape(1, 1, members * tile)


def solution(mesh):
    return jax.shard_map(
        local,
        mesh=mesh,
        in_specs=(P("mrow", "pcol"), P("pcol")),
        out_specs=P("mrow", "pcol", None),
        check_vma=False,
    )
```

```python
import jax
import jax.numpy as jnp
from jax import lax
from jax.experimental import pallas as pl
from jax.experimental.pallas import tpu as pltpu
from jax.sharding import PartitionSpec as P

MEMBERS = 7424
MESH = pl.DeviceIdType.MESH
SENDS = 80


def device(x, y, p, lo, core):
    return (y * 2 + lo, x * 8 + p * 2 + core)


def kernel(
    x_ref, w_ref, out_ref, rows, cols, passing, sums, ysums, table, part, peer,
    row_sem, col_sem, pass_sem, sum_sem, ysum_sem, ztab_sem, xtab_sem, peer_sem, send_sem, load_sem, store_sem,
):
    half = rows.shape[1] // 2
    tile = half // 2
    me_row, me_col = lax.axis_index("mrow"), lax.axis_index("pcol")
    y, lo = me_row // 2, me_row % 2
    x, p, core = me_col // 8, (me_col // 2) % 4, me_col % 2
    hi = p // 2

    xp, xm, x2 = (x + 1) % 4, (x + 3) % 4, (x + 2) % 4
    pp, pm, p2 = (p + 1) % 4, (p + 3) % 4, (p + 2) % 4
    yp, ym, y2 = (y + 1) % 4, (y + 3) % 4, (y + 2) % 4
    x_plus, x_minus, x_far = (device(v, y, p, lo, core) for v in (xp, xm, x2))
    z_plus, z_minus, z_far = (device(x, y, v, lo, core) for v in (pp, pm, p2))
    y_plus, y_minus, y_far = (device(x, v, p, lo, core) for v in (yp, ym, y2))
    z_pair = device(x, y, p, 1 - lo, core)
    twin = device(x, y, p, lo, 1 - core)
    own = x * 4 + p
    diagonal = x == y

    def origin(v):
        return (v + 2 * ((x + v + 1) % 2)) % 4


    turn_lo = [((lo + s - p) % 4) // 2 for s in range(2)]
    turned = [device(x, y, 2 * lo + s, turn_lo[s], core) for s in range(2)]
    stays = [2 * lo + s == p for s in range(2)]
    moves = [jnp.logical_not(v) for v in stays]
    first_p = [(p - hi - 3 * lo) % 4, (p - hi - 1 - lo) % 4]
    second_p = [(p - hi - 3 * (1 - lo)) % 4, (p - hi - 2 + lo) % 4]
    turn_from = [device(x, y, q, hi, core) for q in first_p]
    from_here = [(q == p) & (hi == lo) for q in first_p]
    ahead, behind = hi == lo, hi != lo
    early_p = [jnp.where(ahead, a, b) for a, b in zip(first_p, second_p)]
    late_p = [jnp.where(ahead, b, a) for a, b in zip(first_p, second_p)]

    load = pltpu.make_async_copy(x_ref, rows.at[own], load_sem)
    load.start()
    barrier = pltpu.get_barrier_semaphore()

    def greet(dev):
        pl.semaphore_signal(barrier, inc=1, device_id=dev, device_id_type=MESH)

    for dev in (x_plus, x_minus, x_far, z_plus, z_minus, z_far, y_plus, y_minus, y_far, z_pair, twin):
        greet(dev)
    for s in range(2):
        @pl.when(jnp.logical_not(from_here[s]))
        def _():
            greet(turn_from[s])

    load.wait()
    sums[pl.ds(0, 1)] = jnp.sum(rows[own].astype(jnp.float32), axis=0, keepdims=True)[None]
    pl.semaphore_wait(barrier, 13 - jnp.where(hi == lo, 1, 0))

    sems, sent = {}, {}
    part_of = ["all"]

    def sem_of(name):
        return sems.setdefault(name, len(sems))

    def copy_to(src, dst, recv_sem, dev, n):
        return pltpu.make_async_remote_copy(
            src_ref=src, dst_ref=dst, send_sem=send_sem.at[n], recv_sem=recv_sem,
            device_id=dev, device_id_type=MESH,
        )

    def send(name, src, dst, recv_sem, dev):
        copy_to(src, dst, recv_sem, dev, sem_of(name)).start()
        sent.setdefault(name, set()).add(part_of[0])

    small = []

    def send_small(src, dst, recv_sem, dev):
        copy = copy_to(src, dst, recv_sem, dev, sem_of(("small", len(small))))
        copy.start()
        small.append(copy)

    def arrived(ref, recv_sem):
        copy_to(ref, ref, recv_sem, twin, 0).wait_recv()

    def row_half(i, s):
        return rows.at[i, pl.ds(s * half, half)]

    def send_row(name, i, s, way):
        dev = {"x+": x_plus, "x-": x_minus, "z+": z_plus, "z-": z_minus}[way]
        send((name, s, way), row_half(i, s), row_half(i, s), row_sem.at[i, s], dev)

    def row_arrived(i, s):
        arrived(row_half(i, s), row_sem.at[i, s])

    def send_col(name, i, way):
        dev = {"y+": y_plus, "y-": y_minus, "pair": z_pair}[way]
        send((name, way), cols.at[i], cols.at[i], col_sem.at[i], dev)

    def col_arrived(i):
        arrived(cols.at[i], col_sem.at[i])

    def x_forward(name, q, r):
        i, j = xm * 4 + q, xp * 4 + r
        row_arrived(i, 0)
        send_row(name, i, 0, "x+")
        row_arrived(j, 1)
        send_row(name, j, 1, "x-")

    pushes = []

    def push(src, i, s, dev):
        n = sem_of(("push", len(pushes)))

        @pl.when(diagonal & stays[s])
        def _():
            copy_to(src, cols.at[i], col_sem.at[i], dev, n).start()

        @pl.when(diagonal & moves[s])
        def _():
            copy_to(src, passing.at[s], pass_sem.at[s], dev, n).start()

        pushes.append((src, n))

    def push_row(v, s, dev):
        push(row_half(v * 4 + p, s), v * 4 + p, s, dev)

    turns = []

    def turn_on(s):
        n = sem_of(("turn", s))
        i = origin(y) * 4 + p

        @pl.when(diagonal & moves[s])
        def _():
            copy_to(row_half(x2 * 4 + p, s), cols.at[i], col_sem.at[i], turned[s], n).start()

        @pl.when(diagonal & stays[s])
        def _():
            cols[pl.ds(i, 1)] = rows[pl.ds(x2 * 4 + p, 1), s * half:(s + 1) * half]

        @pl.when(jnp.logical_not(diagonal) & moves[s])
        def _():
            arrived(passing.at[s], pass_sem.at[s])
            copy_to(passing.at[s], cols.at[i], col_sem.at[i], turned[s], n).start()

        turns.append((s, n))

    def to_anomaly(block, i):
        entry = table[i]
        return ((block.astype(jnp.float32) - entry[0:1]) * entry[1:2]).astype(jnp.bfloat16)

    contract = (((1,), (1,)), ((), ()))

    def nth(n, values):
        value = values[0]
        for k in range(1, len(values)):
            value = jnp.where(n == k, values[k], value)
        return value

    def start():
        send_small(sums.at[0], sums.at[1], sum_sem, z_pair)
        send_row("own", own, 0, "x+")
        send_row("own", own, 1, "x-")
        send_row("own", own, 0, "z+")
        send_row("own", own, 1, "z-")
        send_row("own", own, 1, "x+")
        send_row("own", own, 0, "x-")

    def pair_sums():
        arrived(sums.at[1], sum_sem)
        ysums[pl.ds(y, 1)] = (sums[0] + sums[1])[None]
        for dev in (y_plus, y_minus, y_far):
            send_small(ysums.at[y], ysums.at[y], ysum_sem.at[y], dev)
        push_row(x, 0, y_far)
        push_row(x, 1, y_far)

    def means():
        for v in (yp, ym, y2):
            arrived(ysums.at[v], ysum_sem.at[v])
        mean = jnp.sum(ysums[...], axis=0) / MEMBERS
        table[pl.ds(own, 1)] = jnp.concatenate([mean, jnp.sqrt(w_ref[...])], axis=0)[None]
        for dev in (z_plus, z_minus, z_far):
            send_small(table.at[own], table.at[own], ztab_sem.at[p], dev)
        send_row("own", own, 1, "z+")
        send_row("own", own, 0, "z-")

    def x_fwd0():
        x_forward("fwd0", p, p)

    def near_push():
        push_row(xm, 0, y_minus)
        push_row(xp, 1, y_plus)

    def z_first():
        i, j = x * 4 + pm, x * 4 + pp
        row_arrived(i, 0)
        send_row("minus", i, 0, "x+")
        row_arrived(j, 1)
        send_row("plus", j, 1, "x-")
        send_row("plus", j, 1, "x+")
        send_row("minus", i, 0, "x-")

    def z_fwd():
        send_row("minus", x * 4 + pm, 0, "z+")
        send_row("plus", x * 4 + pp, 1, "z-")

    def near_push2():
        row_arrived(xm * 4 + p, 1)
        push_row(xm, 1, y_minus)
        row_arrived(xp * 4 + p, 0)
        push_row(xp, 0, y_plus)

    def tables():
        for q in (pp, pm, p2):
            arrived(table.at[x * 4 + q], ztab_sem.at[q])
        group = table.at[pl.ds(x * 4, 4)]
        for dev in (x_plus, x_minus, x_far):
            send_small(group, group, xtab_sem.at[x], dev)

    def far_rows():
        row_arrived(x2 * 4 + p, 0)
        row_arrived(x2 * 4 + p, 1)

    def z_second():
        i, j = x * 4 + pm, x * 4 + pp
        row_arrived(j, 0)
        send_row("plus", j, 0, "x+")
        row_arrived(i, 1)
        send_row("minus", i, 1, "x-")
        send_row("minus", i, 1, "x+")
        send_row("plus", j, 0, "x-")

    def turn0():
        turn_on(0)

    def turn1():
        turn_on(1)

    def x_fwd1a():
        x_forward("fwd1a", pm, pp)

    def x_fwd1b():
        x_forward("fwd1b", pp, pm)

    def x_fwd2():
        x_forward("fwd2", p2, p2)

    def early(s):
        i = origin(y) * 4 + early_p[s]

        @pl.when(jnp.logical_not(from_here[s] & diagonal))
        def _():
            col_arrived(i)

        if part_of[0] == "ahead":
            send_col(("early", s), i, "pair")
        send_col(("early", s), i, "y+")
        send_col(("early", s), i, "y-")

    def late(s):
        i = origin(y) * 4 + late_p[s]
        col_arrived(i)
        if part_of[0] == "behind":
            send_col(("late", s), i, "pair")
        send_col(("late", s), i, "y+")
        send_col(("late", s), i, "y-")

    def early0():
        early(0)

    def early1():
        early(1)

    def late0():
        late(0)

    def late1():
        late(1)

    def z_far_rows():
        k = x * 4 + p2
        row_arrived(k, 0)
        send_row("far", k, 0, "x+")
        row_arrived(k, 1)
        send_row("far", k, 1, "x-")
        send_row("far", k, 1, "x+")
        send_row("far", k, 0, "x-")

    def tables2():
        for v in (xp, xm, x2):
            arrived(table.at[pl.ds(v * 4, 4)], xtab_sem.at[v])

    def early_fwd():
        i, j = origin(ym) * 4 + early_p[0], origin(yp) * 4 + early_p[1]
        col_arrived(i)
        if part_of[0] == "ahead":
            send_col("early_fwd", i, "y+")
        col_arrived(j)
        if part_of[0] == "ahead":
            send_col("early_fwd", j, "y-")

    def early_pass():
        for s in range(2):
            i = origin(y2) * 4 + early_p[s]
            col_arrived(i)
            if part_of[0] == "ahead":
                send_col(("early_pass", s), i, "pair")

    def late_fwd():
        i, j = origin(ym) * 4 + late_p[0], origin(yp) * 4 + late_p[1]
        col_arrived(i)
        send_col("late_fwd", i, "y+")
        col_arrived(j)
        send_col("late_fwd", j, "y-")

    def rows_rest(q):
        row_arrived(x2 * 4 + q, 0)
        row_arrived(x2 * 4 + q, 1)

    def rows_near():
        for q in (pm, pp):
            row_arrived(xm * 4 + q, 1)
            row_arrived(xp * 4 + q, 0)

    def rows_next():
        rows_rest(pm)
        rows_rest(pp)

    def rows_far():
        row_arrived(xm * 4 + p2, 1)
        row_arrived(xp * 4 + p2, 0)

    e0, e1 = early_p
    l0, l1 = late_p

    def products(blocks, wanted, wait=False):
        def product(n, _):
            i = nth(n, [origin(v) * 4 + q for v, q in blocks])
            if wait:
                col_arrived(i)

            @pl.when(wanted(i // 4, i % 4))
            def _():
                block = to_anomaly(rows[i], i)
                column = to_anomaly(cols[i], i)
                for c in range(2):
                    part[c] += lax.dot_general(
                        block, column[c * tile:(c + 1) * tile], contract,
                        preferred_element_type=jnp.float32,
                    )
            return 0

        lax.fori_loop(0, len(blocks), product, 0)

    def now(v, q):
        return (q != p2) & ((q == p) | (v != x2))

    def next_(v, q):
        return (q != p2) & (q != p) & (v == x2)

    def near(v, q):
        return q != p2

    def far(v, q):
        return (q == p2) & (v != x2)

    own_early, own_late = ((y, e0), (y, e1)), ((y, l0), (y, l1))
    side_early, side_early2 = ((ym, e0), (yp, e1)), ((ym, e1), (yp, e0))
    side_late, side_late2 = ((ym, l0), (yp, l1)), ((ym, l1), (yp, l0))
    far_early, far_late = ((y2, e0), (y2, e1)), ((y2, l0), (y2, l1))

    def clear():
        part[...] = jnp.zeros_like(part)

    def a1():
        for q in (e1, e0):
            col_arrived(origin(ym if q is e1 else yp) * 4 + q)
        rows_near()
        products(own_early + side_early + side_early2 + far_early, now)

    def a2():
        rows_next()
        products(own_early + side_early + side_early2 + far_early, next_)
        products(own_late, near)

    def a3():
        products(side_late, near)

    def b1():
        rows_near()
        products(own_late + own_early, now)

    def b2():
        rows_next()
        products(own_late + own_early, next_)
        products(side_late + side_early, near)

    def b3():
        products(side_late2 + side_early2, near, True)

    def b4():
        products(far_early, near)

    def not_last(v, q):
        return (q != p2) | (v != x2)

    def a_far():
        rows_far()
        products(own_early + side_early + side_early2 + far_early + own_late + side_late, far)

    def a_rest():
        products(side_late2 + far_late, not_last, True)

    def b_far():
        rows_far()
        products(own_early + side_early + side_early2 + far_early + own_late + side_late + side_late2, far)

    def b_rest():
        products(far_late, not_last, True)

    def last():
        i = x2 * 4 + p2
        column = to_anomaly(cols[i], i)
        tiles = column[:tile], column[tile:]
        theirs = jnp.where(core == 0, tiles[1], tiles[0])
        mine = jnp.where(core == 0, tiles[0], tiles[1])

        def halves(s):
            return pl.ds(s * half, half)

        def term(s, right):
            block = to_anomaly(rows[i, s * half:(s + 1) * half], i)
            return lax.dot_general(block, right, contract, preferred_element_type=jnp.float32)

        for s in range(2):
            row_arrived(i, s)
            part[1 - core, halves(s)] += term(s, theirs)
        for s in range(2):
            send_small(part.at[1 - core, halves(s)], peer.at[halves(s)], peer_sem.at[s], twin)
            part[core, halves(s)] += term(s, mine)
        stores = []
        for s in range(2):
            arrived(peer.at[halves(s)], peer_sem.at[s])
            part[core, halves(s)] = (part[core, halves(s)] + peer[halves(s)]) * (1.0 / (MEMBERS - 1))
            stores.append(pltpu.make_async_copy(part.at[core, halves(s)], out_ref.at[halves(s)], store_sem.at[s]))
            stores[s].start()
        for store in stores:
            store.wait()

    def run(steps):
        for step in steps:
            step()

    run((start, pair_sums, means, clear, x_fwd0, near_push, near_push2, z_first, far_rows, turn0, turn1, tables, z_second, x_fwd1a,))

    @pl.when(ahead)
    def _():
        part_of[0] = "ahead"
        run((early0, early1, z_fwd, x_fwd1b, early_fwd, early_pass, tables2, a1, z_far_rows, late0, late1, x_fwd2, a2, late_fwd, a3, a_far, a_rest,))

    @pl.when(behind)
    def _():
        part_of[0] = "behind"
        run((z_fwd, x_fwd1b, early0, late0, late1, early1, z_far_rows, late_fwd, tables2, b1, x_fwd2, early_fwd, b2, b3, early_pass, b4, b_far, b_rest,))

    part_of[0] = "all"
    run((last,))

    for copy in small:
        copy.wait_send()

    def left(name):
        copy_to(cols.at[0], cols.at[0], pass_sem.at[0], twin, sems[name]).wait_send()

    for name, parts in sent.items():
        if parts == {"ahead"}:
            pl.when(ahead)(lambda name=name: left(name))
        elif parts == {"behind"}:
            pl.when(behind)(lambda name=name: left(name))
        else:
            left(name)
    for src, n in pushes:
        @pl.when(diagonal)
        def _():
            copy_to(src, src, pass_sem.at[0], twin, n).wait_send()
    for s, n in turns:
        @pl.when(moves[s])
        def _():
            copy_to(passing.at[s], passing.at[s], pass_sem.at[0], twin, n).wait_send()


def local(snapshots, area_weight):
    members, points = snapshots.shape
    tile = members // 4
    vmem = pl.BlockSpec(memory_space=pltpu.VMEM)
    hbm = pl.BlockSpec(memory_space=pl.ANY)
    dma = pltpu.SemaphoreType.DMA
    gram = pl.pallas_call(
        kernel,
        out_shape=jax.ShapeDtypeStruct((members, tile), jnp.float32),
        in_specs=[hbm, vmem],
        out_specs=hbm,
        scratch_shapes=[
            pltpu.VMEM((16, members, points), jnp.bfloat16),
            pltpu.VMEM((16, members // 2, points), jnp.bfloat16),
            pltpu.VMEM((2, members // 2, points), jnp.bfloat16),
            pltpu.VMEM((2, 1, points), jnp.float32),
            pltpu.VMEM((4, 1, points), jnp.float32),
            pltpu.VMEM((16, 2, points), jnp.float32),
            pltpu.VMEM((2, members, tile), jnp.float32),
            pltpu.VMEM((members, tile), jnp.float32),
            dma((16, 2)),
            dma((16,)),
            dma((2,)),
            dma,
            dma((4,)),
            dma((4,)),
            dma((4,)),
            dma((2,)),
            dma((SENDS,)),
            dma,
            dma((2,)),
        ],
        compiler_params=pltpu.CompilerParams(collective_id=0, has_side_effects=True),
    )(snapshots, area_weight.reshape(1, points))
    return gram.reshape(1, 1, members * tile)


def solution(mesh):
    return jax.shard_map(
        local,
        mesh=mesh,
        in_specs=(P("mrow", "pcol"), P("pcol")),
        out_specs=P("mrow", "pcol", None),
        check_vma=False,
    )
```

```python
import jax
import jax.numpy as jnp
from jax import lax
from jax.experimental import pallas as pl
from jax.experimental.pallas import tpu as pltpu
from jax.sharding import PartitionSpec as P

MEMBERS = 7424
MESH = pl.DeviceIdType.MESH
SENDS = 80


def device(x, y, p, lo, core):
    return (y * 2 + lo, x * 8 + p * 2 + core)


def kernel(
    x_ref, w_ref, out_ref, rows, cols, passing, sums, ysums, table, part, peer,
    row_sem, col_sem, pass_sem, sum_sem, ysum_sem, ztab_sem, xtab_sem, peer_sem, send_sem,
):
    half = rows.shape[1] // 2
    tile = half // 2
    me_row, me_col = lax.axis_index("mrow"), lax.axis_index("pcol")
    y, lo = me_row // 2, me_row % 2
    x, p, core = me_col // 8, (me_col // 2) % 4, me_col % 2
    hi = p // 2

    xp, xm, x2 = (x + 1) % 4, (x + 3) % 4, (x + 2) % 4
    pp, pm, p2 = (p + 1) % 4, (p + 3) % 4, (p + 2) % 4
    yp, ym, y2 = (y + 1) % 4, (y + 3) % 4, (y + 2) % 4
    x_plus, x_minus, x_far = (device(v, y, p, lo, core) for v in (xp, xm, x2))
    z_plus, z_minus, z_far = (device(x, y, v, lo, core) for v in (pp, pm, p2))
    y_plus, y_minus, y_far = (device(x, v, p, lo, core) for v in (yp, ym, y2))
    z_pair = device(x, y, p, 1 - lo, core)
    twin = device(x, y, p, lo, 1 - core)
    own = x * 4 + p
    diagonal = x == y

    def origin(v):
        return (v + 2 * ((x + v + 1) % 2)) % 4


    turn_lo = [((lo + s - p) % 4) // 2 for s in range(2)]
    turned = [device(x, y, 2 * lo + s, turn_lo[s], core) for s in range(2)]
    stays = [2 * lo + s == p for s in range(2)]
    moves = [jnp.logical_not(v) for v in stays]
    first_p = [(p - hi - 3 * lo) % 4, (p - hi - 1 - lo) % 4]
    second_p = [(p - hi - 3 * (1 - lo)) % 4, (p - hi - 2 + lo) % 4]
    turn_from = [device(x, y, q, hi, core) for q in first_p]
    from_here = [(q == p) & (hi == lo) for q in first_p]
    ahead, behind = hi == lo, hi != lo
    early_p = [jnp.where(ahead, a, b) for a, b in zip(first_p, second_p)]
    late_p = [jnp.where(ahead, b, a) for a, b in zip(first_p, second_p)]

    barrier = pltpu.get_barrier_semaphore()

    def greet(dev):
        pl.semaphore_signal(barrier, inc=1, device_id=dev, device_id_type=MESH)

    for dev in (x_plus, x_minus, x_far, z_plus, z_minus, z_far, y_plus, y_minus, y_far, z_pair, twin):
        greet(dev)
    for s in range(2):
        @pl.when(jnp.logical_not(from_here[s]))
        def _():
            greet(turn_from[s])

    sums[pl.ds(0, 1)] = jnp.sum(x_ref[...].astype(jnp.float32), axis=0, keepdims=True)[None]
    pl.semaphore_wait(barrier, 13 - jnp.where(hi == lo, 1, 0))

    sems, sent = {}, {}
    part_of = ["all"]

    def sem_of(name):
        return sems.setdefault(name, len(sems))

    def copy_to(src, dst, recv_sem, dev, n):
        return pltpu.make_async_remote_copy(
            src_ref=src, dst_ref=dst, send_sem=send_sem.at[n], recv_sem=recv_sem,
            device_id=dev, device_id_type=MESH,
        )

    def send(name, src, dst, recv_sem, dev):
        copy_to(src, dst, recv_sem, dev, sem_of(name)).start()
        sent.setdefault(name, set()).add(part_of[0])

    small = []

    def send_small(src, dst, recv_sem, dev):
        copy = copy_to(src, dst, recv_sem, dev, sem_of(("small", len(small))))
        copy.start()
        small.append(copy)

    def arrived(ref, recv_sem):
        copy_to(ref, ref, recv_sem, twin, 0).wait_recv()

    def row_half(i, s):
        return rows.at[i, pl.ds(s * half, half)]

    def send_row(name, i, s, way):
        dev = {"x+": x_plus, "x-": x_minus, "z+": z_plus, "z-": z_minus}[way]
        send((name, s, way), row_half(i, s), row_half(i, s), row_sem.at[i, s], dev)

    def row_arrived(i, s):
        arrived(row_half(i, s), row_sem.at[i, s])

    def own_half(s):
        return x_ref.at[pl.ds(s * half, half)]

    def send_own(s, way):
        dev = {"x+": x_plus, "x-": x_minus, "z+": z_plus, "z-": z_minus}[way]
        send(("own", s, way), own_half(s), row_half(own, s), row_sem.at[own, s], dev)

    def send_col(name, i, way):
        dev = {"y+": y_plus, "y-": y_minus, "pair": z_pair}[way]
        send((name, way), cols.at[i], cols.at[i], col_sem.at[i], dev)

    def col_arrived(i):
        arrived(cols.at[i], col_sem.at[i])

    def x_forward(name, q, r):
        i, j = xm * 4 + q, xp * 4 + r
        row_arrived(i, 0)
        send_row(name, i, 0, "x+")
        row_arrived(j, 1)
        send_row(name, j, 1, "x-")

    pushes = []

    def push(src, i, s, dev):
        n = sem_of(("push", len(pushes)))

        @pl.when(diagonal & stays[s])
        def _():
            copy_to(src, cols.at[i], col_sem.at[i], dev, n).start()

        @pl.when(diagonal & moves[s])
        def _():
            copy_to(src, passing.at[s], pass_sem.at[s], dev, n).start()

        pushes.append((src, n))

    def push_row(v, s, dev):
        push(row_half(v * 4 + p, s), v * 4 + p, s, dev)

    turns = []

    def turn_on(s):
        n = sem_of(("turn", s))
        i = origin(y) * 4 + p

        @pl.when(diagonal & moves[s])
        def _():
            copy_to(row_half(x2 * 4 + p, s), cols.at[i], col_sem.at[i], turned[s], n).start()

        @pl.when(diagonal & stays[s])
        def _():
            cols[pl.ds(i, 1)] = rows[pl.ds(x2 * 4 + p, 1), s * half:(s + 1) * half]

        @pl.when(jnp.logical_not(diagonal) & moves[s])
        def _():
            arrived(passing.at[s], pass_sem.at[s])
            copy_to(passing.at[s], cols.at[i], col_sem.at[i], turned[s], n).start()

        turns.append((s, n))

    def to_anomaly(block, i):
        entry = table[i]
        return ((block.astype(jnp.float32) - entry[0:1]) * entry[1:2]).astype(jnp.bfloat16)

    contract = (((1,), (1,)), ((), ()))

    def nth(n, values):
        value = values[0]
        for k in range(1, len(values)):
            value = jnp.where(n == k, values[k], value)
        return value

    def start():
        send_small(sums.at[0], sums.at[1], sum_sem, z_pair)
        send_own(0, "x+")
        send_own(1, "x-")
        send_own(0, "z+")
        send_own(1, "z-")
        send_own(1, "x+")
        send_own(0, "x-")

    def pair_sums():
        arrived(sums.at[1], sum_sem)
        ysums[pl.ds(y, 1)] = (sums[0] + sums[1])[None]
        for dev in (y_plus, y_minus, y_far):
            send_small(ysums.at[y], ysums.at[y], ysum_sem.at[y], dev)
        push(own_half(0), own, 0, y_far)
        push(own_half(1), own, 1, y_far)

    def means():
        for v in (yp, ym, y2):
            arrived(ysums.at[v], ysum_sem.at[v])
        mean = jnp.sum(ysums[...], axis=0) / MEMBERS
        table[pl.ds(own, 1)] = jnp.concatenate([mean, jnp.sqrt(w_ref[...])], axis=0)[None]
        for dev in (z_plus, z_minus, z_far):
            send_small(table.at[own], table.at[own], ztab_sem.at[p], dev)
        send_own(1, "z+")
        send_own(0, "z-")

    def x_fwd0():
        x_forward("fwd0", p, p)

    def near_push():
        push_row(xm, 0, y_minus)
        push_row(xp, 1, y_plus)

    def z_first():
        i, j = x * 4 + pm, x * 4 + pp
        row_arrived(i, 0)
        send_row("minus", i, 0, "x+")
        row_arrived(j, 1)
        send_row("plus", j, 1, "x-")
        send_row("plus", j, 1, "x+")
        send_row("minus", i, 0, "x-")

    def z_fwd():
        send_row("minus", x * 4 + pm, 0, "z+")
        send_row("plus", x * 4 + pp, 1, "z-")

    def near_push2():
        row_arrived(xm * 4 + p, 1)
        push_row(xm, 1, y_minus)
        row_arrived(xp * 4 + p, 0)
        push_row(xp, 0, y_plus)

    def tables():
        for q in (pp, pm, p2):
            arrived(table.at[x * 4 + q], ztab_sem.at[q])
        group = table.at[pl.ds(x * 4, 4)]
        for dev in (x_plus, x_minus, x_far):
            send_small(group, group, xtab_sem.at[x], dev)

    def far_rows():
        row_arrived(x2 * 4 + p, 0)
        row_arrived(x2 * 4 + p, 1)

    def z_second():
        i, j = x * 4 + pm, x * 4 + pp
        row_arrived(j, 0)
        send_row("plus", j, 0, "x+")
        row_arrived(i, 1)
        send_row("minus", i, 1, "x-")
        send_row("minus", i, 1, "x+")
        send_row("plus", j, 0, "x-")

    def turn0():
        turn_on(0)

    def turn1():
        turn_on(1)

    def x_fwd1a():
        x_forward("fwd1a", pm, pp)

    def x_fwd1b():
        x_forward("fwd1b", pp, pm)

    def x_fwd2():
        x_forward("fwd2", p2, p2)

    def early(s):
        i = origin(y) * 4 + early_p[s]

        @pl.when(jnp.logical_not(from_here[s] & diagonal))
        def _():
            col_arrived(i)

        if part_of[0] == "ahead":
            send_col(("early", s), i, "pair")
        send_col(("early", s), i, "y+")
        send_col(("early", s), i, "y-")

    def late(s):
        i = origin(y) * 4 + late_p[s]
        col_arrived(i)
        if part_of[0] == "behind":
            send_col(("late", s), i, "pair")
        send_col(("late", s), i, "y+")
        send_col(("late", s), i, "y-")

    def early0():
        early(0)

    def early1():
        early(1)

    def late0():
        late(0)

    def late1():
        late(1)

    def z_far_rows():
        k = x * 4 + p2
        row_arrived(k, 0)
        send_row("far", k, 0, "x+")
        row_arrived(k, 1)
        send_row("far", k, 1, "x-")
        send_row("far", k, 1, "x+")
        send_row("far", k, 0, "x-")

    def tables2():
        for v in (xp, xm, x2):
            arrived(table.at[pl.ds(v * 4, 4)], xtab_sem.at[v])

    def early_fwd():
        i, j = origin(ym) * 4 + early_p[0], origin(yp) * 4 + early_p[1]
        col_arrived(i)
        if part_of[0] == "ahead":
            send_col("early_fwd", i, "y+")
        col_arrived(j)
        if part_of[0] == "ahead":
            send_col("early_fwd", j, "y-")

    def early_pass():
        for s in range(2):
            i = origin(y2) * 4 + early_p[s]
            col_arrived(i)
            if part_of[0] == "ahead":
                send_col(("early_pass", s), i, "pair")

    def late_fwd():
        i, j = origin(ym) * 4 + late_p[0], origin(yp) * 4 + late_p[1]
        col_arrived(i)
        send_col("late_fwd", i, "y+")
        col_arrived(j)
        send_col("late_fwd", j, "y-")

    def rows_rest(q):
        row_arrived(x2 * 4 + q, 0)
        row_arrived(x2 * 4 + q, 1)

    def rows_near():
        for q in (pm, pp):
            row_arrived(xm * 4 + q, 1)
            row_arrived(xp * 4 + q, 0)

    def rows_next():
        rows_rest(pm)
        rows_rest(pp)

    def rows_far():
        row_arrived(xm * 4 + p2, 1)
        row_arrived(xp * 4 + p2, 0)

    e0, e1 = early_p
    l0, l1 = late_p

    def products(blocks, wanted, wait=False):
        def product(n, _):
            i = nth(n, [origin(v) * 4 + q for v, q in blocks])
            if wait:
                col_arrived(i)

            @pl.when(wanted(i // 4, i % 4))
            def _():
                block = to_anomaly(rows[i], i)
                column = to_anomaly(cols[i], i)
                for c in range(2):
                    part[c] += lax.dot_general(
                        block, column[c * tile:(c + 1) * tile], contract,
                        preferred_element_type=jnp.float32,
                    )
            return 0

        lax.fori_loop(0, len(blocks), product, 0)

    def now(v, q):
        return (q != p2) & ((q == p) | (v != x2))

    def next_(v, q):
        return (q != p2) & (q != p) & (v == x2)

    def near(v, q):
        return q != p2

    def far(v, q):
        return (q == p2) & (v != x2)

    own_early, own_late = ((y, e0), (y, e1)), ((y, l0), (y, l1))
    side_early, side_early2 = ((ym, e0), (yp, e1)), ((ym, e1), (yp, e0))
    side_late, side_late2 = ((ym, l0), (yp, l1)), ((ym, l1), (yp, l0))
    far_early, far_late = ((y2, e0), (y2, e1)), ((y2, l0), (y2, l1))

    def clear():
        part[...] = jnp.zeros_like(part)
        rows[pl.ds(own, 1)] = x_ref[...][None]

    def a1():
        for q in (e1, e0):
            col_arrived(origin(ym if q is e1 else yp) * 4 + q)
        rows_near()
        products(own_early + side_early + side_early2 + far_early, now)

    def a2():
        rows_next()
        products(own_early + side_early + side_early2 + far_early, next_)
        products(own_late, near)

    def a3():
        products(side_late, near)

    def b1():
        rows_near()
        products(own_late + own_early, now)

    def b2():
        rows_next()
        products(own_late + own_early, next_)
        products(side_late + side_early, near)

    def b3():
        products(side_late2 + side_early2, near, True)

    def b4():
        products(far_early, near)

    def not_last(v, q):
        return (q != p2) | (v != x2)

    def a_far():
        rows_far()
        products(own_early + side_early + side_early2 + far_early + own_late + side_late, far)

    def a_rest():
        products(side_late2 + far_late, not_last, True)

    def b_far():
        rows_far()
        products(own_early + side_early + side_early2 + far_early + own_late + side_late + side_late2, far)

    def b_rest():
        products(far_late, not_last, True)

    def last():
        i = x2 * 4 + p2
        column = to_anomaly(cols[i], i)
        tiles = column[:tile], column[tile:]
        theirs = jnp.where(core == 0, tiles[1], tiles[0])
        mine = jnp.where(core == 0, tiles[0], tiles[1])

        def halves(s):
            return pl.ds(s * half, half)

        def term(s, right):
            block = to_anomaly(rows[i, s * half:(s + 1) * half], i)
            return lax.dot_general(block, right, contract, preferred_element_type=jnp.float32)

        for s in range(2):
            row_arrived(i, s)
            part[1 - core, halves(s)] += term(s, theirs)
        for s in range(2):
            send_small(part.at[1 - core, halves(s)], peer.at[halves(s)], peer_sem.at[s], twin)
            part[core, halves(s)] += term(s, mine)
        for s in range(2):
            arrived(peer.at[halves(s)], peer_sem.at[s])
            out_ref[halves(s)] = (part[core, halves(s)] + peer[halves(s)]) * (1.0 / (MEMBERS - 1))

    def left(name):
        copy_to(cols.at[0], cols.at[0], pass_sem.at[0], twin, sems[name]).wait_send()

    def made(name, kind):
        return name not in drained[kind] and bool(sent[name] & {"all", kind})

    drained = {"ahead": set(), "behind": set()}

    def drain(names):
        for name in names:
            if made(name, part_of[0]):
                left(name)
                drained[part_of[0]].add(name)

    def drain_first():
        drain([name for name in sent if "all" in sent[name]])
        for copy in small[:10]:
            copy.wait_send()
        for src, n in pushes:
            @pl.when(diagonal)
            def _():
                copy_to(src, src, pass_sem.at[0], twin, n).wait_send()
        for s, n in turns:
            @pl.when(moves[s])
            def _():
                copy_to(passing.at[s], passing.at[s], pass_sem.at[0], twin, n).wait_send()

    def drain_second():
        drain([name for name in sent if name[0] not in ("far", "fwd2", ("late", 0), ("late", 1), "late_fwd")])

    def run(steps):
        for step in steps:
            step()

    run((start, pair_sums, means, clear, x_fwd0, near_push, near_push2, z_first, far_rows, turn0, turn1, tables, z_second, x_fwd1a,))

    @pl.when(ahead)
    def _():
        part_of[0] = "ahead"
        run((early0, early1, z_fwd, x_fwd1b, early_fwd, early_pass, tables2, a1, z_far_rows, late0, late1, x_fwd2, drain_first, a2, late_fwd, a3, a_far, drain_second, a_rest,))

    @pl.when(behind)
    def _():
        part_of[0] = "behind"
        run((z_fwd, x_fwd1b, early0, late0, late1, early1, z_far_rows, late_fwd, tables2, b1, x_fwd2, drain_first, early_fwd, b2, b3, early_pass, b4, b_far, drain_second, b_rest,))

    part_of[0] = "all"
    run((last,))

    for copy in small[10:]:
        copy.wait_send()
    for name in sent:
        kinds = [kind for kind in drained if made(name, kind)]
        if len(kinds) == 2:
            left(name)
        elif kinds:
            pl.when(ahead if kinds == ["ahead"] else behind)(lambda name=name: left(name))


def local(snapshots, area_weight):
    members, points = snapshots.shape
    tile = members // 4
    vmem = pl.BlockSpec(memory_space=pltpu.VMEM)
    dma = pltpu.SemaphoreType.DMA
    gram = pl.pallas_call(
        kernel,
        out_shape=jax.ShapeDtypeStruct((members, tile), jnp.float32),
        in_specs=[vmem, vmem],
        out_specs=vmem,
        scratch_shapes=[
            pltpu.VMEM((16, members, points), jnp.bfloat16),
            pltpu.VMEM((16, members // 2, points), jnp.bfloat16),
            pltpu.VMEM((2, members // 2, points), jnp.bfloat16),
            pltpu.VMEM((2, 1, points), jnp.float32),
            pltpu.VMEM((4, 1, points), jnp.float32),
            pltpu.VMEM((16, 2, points), jnp.float32),
            pltpu.VMEM((2, members, tile), jnp.float32),
            pltpu.VMEM((members, tile), jnp.float32),
            dma((16, 2)),
            dma((16,)),
            dma((2,)),
            dma,
            dma((4,)),
            dma((4,)),
            dma((4,)),
            dma((2,)),
            dma((SENDS,)),
        ],
        compiler_params=pltpu.CompilerParams(
            collective_id=0, has_side_effects=True, vmem_limit_bytes=24 * 1024 * 1024
        ),
    )(snapshots, area_weight.reshape(1, points))
    return gram.reshape(1, 1, members * tile)


def solution(mesh):
    return jax.shard_map(
        local,
        mesh=mesh,
        in_specs=(P("mrow", "pcol"), P("pcol")),
        out_specs=P("mrow", "pcol", None),
        check_vma=False,
    )
```

```python
import jax
import jax.numpy as jnp
from jax import lax
from jax.experimental import pallas as pl
from jax.experimental.pallas import tpu as pltpu
from jax.sharding import PartitionSpec as P

MEMBERS = 7424
MESH = pl.DeviceIdType.MESH
SENDS = 18


def device(x, y, p, lo, core):
    return (y * 2 + lo, x * 8 + p * 2 + core)


def kernel(
    x_ref, w_ref, out_ref, rows, cols, passing, sums, ysums, table, part, peer,
    row_sem, col_sem, pass_sem, sum_sem, ysum_sem, ztab_sem, xtab_sem, peer_sem, send_sem,
):
    half = rows.shape[1] // 2
    tile = half // 2
    me_row, me_col = lax.axis_index("mrow"), lax.axis_index("pcol")
    y, lo = me_row // 2, me_row % 2
    x, p, core = me_col // 8, (me_col // 2) % 4, me_col % 2
    hi = p // 2

    xp, xm, x2 = (x + 1) % 4, (x + 3) % 4, (x + 2) % 4
    pp, pm, p2 = (p + 1) % 4, (p + 3) % 4, (p + 2) % 4
    yp, ym, y2 = (y + 1) % 4, (y + 3) % 4, (y + 2) % 4
    x_plus, x_minus, x_far = (device(v, y, p, lo, core) for v in (xp, xm, x2))
    z_plus, z_minus, z_far = (device(x, y, v, lo, core) for v in (pp, pm, p2))
    y_plus, y_minus, y_far = (device(x, v, p, lo, core) for v in (yp, ym, y2))
    z_pair = device(x, y, p, 1 - lo, core)
    twin = device(x, y, p, lo, 1 - core)
    own = x * 4 + p
    diagonal = x == y

    def origin(v):
        return (v + 2 * ((x + v + 1) % 2)) % 4


    turn_lo = [((lo + s - p) % 4) // 2 for s in range(2)]
    turned = [device(x, y, 2 * lo + s, turn_lo[s], core) for s in range(2)]
    stays = [2 * lo + s == p for s in range(2)]
    moves = [jnp.logical_not(v) for v in stays]
    first_p = [(p - hi - 3 * lo) % 4, (p - hi - 1 - lo) % 4]
    second_p = [(p - hi - 3 * (1 - lo)) % 4, (p - hi - 2 + lo) % 4]
    turn_from = [device(x, y, q, hi, core) for q in first_p]
    from_here = [(q == p) & (hi == lo) for q in first_p]
    ahead, behind = hi == lo, hi != lo
    early_p = [jnp.where(ahead, a, b) for a, b in zip(first_p, second_p)]
    late_p = [jnp.where(ahead, b, a) for a, b in zip(first_p, second_p)]

    barrier = pltpu.get_barrier_semaphore()

    def greet(dev):
        pl.semaphore_signal(barrier, inc=1, device_id=dev, device_id_type=MESH)

    for dev in (x_plus, x_minus, x_far, z_plus, z_minus, z_far, y_plus, y_minus, y_far, z_pair, twin):
        greet(dev)
    for s in range(2):
        @pl.when(jnp.logical_not(from_here[s]))
        def _():
            greet(turn_from[s])

    sums[pl.ds(0, 1)] = jnp.sum(x_ref[...].astype(jnp.float32), axis=0, keepdims=True)[None]
    pl.semaphore_wait(barrier, 13 - jnp.where(hi == lo, 1, 0))

    FIRST, SECOND, THIRD, PUSH, TURN, SMALL = 0, 1, 2, 3, 4, 6
    started = {}
    part_of = ["all"]

    def copy_to(src, dst, recv_sem, dev, n):
        return pltpu.make_async_remote_copy(
            src_ref=src, dst_ref=dst, send_sem=send_sem.at[n], recv_sem=recv_sem,
            device_id=dev, device_id_type=MESH,
        )

    def send(name, src, dst, recv_sem, dev):
        if part_of[0] == "all":
            n = FIRST
        elif name[0] in ("far", "fwd2", ("late", 0), ("late", 1), "late_fwd"):
            n = THIRD
        else:
            n = SECOND
        copy_to(src, dst, recv_sem, dev, n).start()
        started[part_of[0], n] = started.get((part_of[0], n), 0) + 1

    def all_left(n, halves):
        blocks = rows.at[pl.ds(0, halves // 2)]
        copy_to(blocks, blocks, pass_sem.at[0], twin, n).wait_send()

    small = []

    def send_small(src, dst, recv_sem, dev):
        copy = copy_to(src, dst, recv_sem, dev, SMALL + len(small))
        copy.start()
        small.append(copy)

    def arrived(ref, recv_sem):
        copy_to(ref, ref, recv_sem, twin, 0).wait_recv()

    def row_half(i, s):
        return rows.at[i, pl.ds(s * half, half)]

    def send_row(name, i, s, way):
        dev = {"x+": x_plus, "x-": x_minus, "z+": z_plus, "z-": z_minus}[way]
        send((name, s, way), row_half(i, s), row_half(i, s), row_sem.at[i, s], dev)

    def row_arrived(i, s):
        arrived(row_half(i, s), row_sem.at[i, s])

    def own_half(s):
        return x_ref.at[pl.ds(s * half, half)]

    def send_own(s, way):
        dev = {"x+": x_plus, "x-": x_minus, "z+": z_plus, "z-": z_minus}[way]
        send(("own", s, way), own_half(s), row_half(own, s), row_sem.at[own, s], dev)

    def send_col(name, i, way):
        dev = {"y+": y_plus, "y-": y_minus, "pair": z_pair}[way]
        send((name, way), cols.at[i], cols.at[i], col_sem.at[i], dev)

    def col_arrived(i):
        arrived(cols.at[i], col_sem.at[i])

    def x_forward(name, q, r):
        i, j = xm * 4 + q, xp * 4 + r
        row_arrived(i, 0)
        send_row(name, i, 0, "x+")
        row_arrived(j, 1)
        send_row(name, j, 1, "x-")

    pushes = []

    def push(src, i, s, dev):
        n = PUSH

        @pl.when(diagonal & stays[s])
        def _():
            copy_to(src, cols.at[i], col_sem.at[i], dev, n).start()

        @pl.when(diagonal & moves[s])
        def _():
            copy_to(src, passing.at[s], pass_sem.at[s], dev, n).start()

        pushes.append((src, n))

    def push_row(v, s, dev):
        push(row_half(v * 4 + p, s), v * 4 + p, s, dev)

    turns = []

    def turn_on(s):
        n = TURN + s
        i = origin(y) * 4 + p

        @pl.when(diagonal & moves[s])
        def _():
            copy_to(row_half(x2 * 4 + p, s), cols.at[i], col_sem.at[i], turned[s], n).start()

        @pl.when(diagonal & stays[s])
        def _():
            cols[pl.ds(i, 1)] = rows[pl.ds(x2 * 4 + p, 1), s * half:(s + 1) * half]

        @pl.when(jnp.logical_not(diagonal) & moves[s])
        def _():
            arrived(passing.at[s], pass_sem.at[s])
            copy_to(passing.at[s], cols.at[i], col_sem.at[i], turned[s], n).start()

        turns.append((s, n))

    def to_anomaly(block, i):
        entry = table[i]
        return ((block.astype(jnp.float32) - entry[0:1]) * entry[1:2]).astype(jnp.bfloat16)

    contract = (((1,), (1,)), ((), ()))

    def nth(n, values):
        value = values[0]
        for k in range(1, len(values)):
            value = jnp.where(n == k, values[k], value)
        return value

    def start():
        send_small(sums.at[0], sums.at[1], sum_sem, z_pair)
        send_own(0, "x+")
        send_own(1, "x-")
        send_own(0, "z+")
        send_own(1, "z-")
        send_own(1, "x+")
        send_own(0, "x-")

    def pair_sums():
        arrived(sums.at[1], sum_sem)
        ysums[pl.ds(y, 1)] = (sums[0] + sums[1])[None]
        for dev in (y_plus, y_minus, y_far):
            send_small(ysums.at[y], ysums.at[y], ysum_sem.at[y], dev)
        push(own_half(0), own, 0, y_far)
        push(own_half(1), own, 1, y_far)

    def means():
        for v in (yp, ym, y2):
            arrived(ysums.at[v], ysum_sem.at[v])
        mean = jnp.sum(ysums[...], axis=0) / MEMBERS
        table[pl.ds(own, 1)] = jnp.concatenate([mean, jnp.sqrt(w_ref[...])], axis=0)[None]
        for dev in (z_plus, z_minus, z_far):
            send_small(table.at[own], table.at[own], ztab_sem.at[p], dev)
        send_own(1, "z+")
        send_own(0, "z-")

    def x_fwd0():
        x_forward("fwd0", p, p)

    def near_push():
        push_row(xm, 0, y_minus)
        push_row(xp, 1, y_plus)

    def z_first():
        i, j = x * 4 + pm, x * 4 + pp
        row_arrived(i, 0)
        send_row("minus", i, 0, "x+")
        row_arrived(j, 1)
        send_row("plus", j, 1, "x-")
        send_row("plus", j, 1, "x+")
        send_row("minus", i, 0, "x-")

    def z_fwd():
        send_row("minus", x * 4 + pm, 0, "z+")
        send_row("plus", x * 4 + pp, 1, "z-")

    def near_push2():
        row_arrived(xm * 4 + p, 1)
        push_row(xm, 1, y_minus)
        row_arrived(xp * 4 + p, 0)
        push_row(xp, 0, y_plus)

    def tables():
        for q in (pp, pm, p2):
            arrived(table.at[x * 4 + q], ztab_sem.at[q])
        group = table.at[pl.ds(x * 4, 4)]
        for dev in (x_plus, x_minus, x_far):
            send_small(group, group, xtab_sem.at[x], dev)

    def far_rows():
        row_arrived(x2 * 4 + p, 0)
        row_arrived(x2 * 4 + p, 1)

    def z_second():
        i, j = x * 4 + pm, x * 4 + pp
        row_arrived(j, 0)
        send_row("plus", j, 0, "x+")
        row_arrived(i, 1)
        send_row("minus", i, 1, "x-")
        send_row("minus", i, 1, "x+")
        send_row("plus", j, 0, "x-")

    def turn0():
        turn_on(0)

    def turn1():
        turn_on(1)

    def x_fwd1a():
        x_forward("fwd1a", pm, pp)

    def x_fwd1b():
        x_forward("fwd1b", pp, pm)

    def x_fwd2():
        x_forward("fwd2", p2, p2)

    def early(s):
        i = origin(y) * 4 + early_p[s]

        @pl.when(jnp.logical_not(from_here[s] & diagonal))
        def _():
            col_arrived(i)

        if part_of[0] == "ahead":
            send_col(("early", s), i, "pair")
        send_col(("early", s), i, "y+")
        send_col(("early", s), i, "y-")

    def late(s):
        i = origin(y) * 4 + late_p[s]
        col_arrived(i)
        if part_of[0] == "behind":
            send_col(("late", s), i, "pair")
        send_col(("late", s), i, "y+")
        send_col(("late", s), i, "y-")

    def early0():
        early(0)

    def early1():
        early(1)

    def late0():
        late(0)

    def late1():
        late(1)

    def z_far_rows():
        k = x * 4 + p2
        row_arrived(k, 0)
        send_row("far", k, 0, "x+")
        row_arrived(k, 1)
        send_row("far", k, 1, "x-")
        send_row("far", k, 1, "x+")
        send_row("far", k, 0, "x-")

    def tables2():
        for v in (xp, xm, x2):
            arrived(table.at[pl.ds(v * 4, 4)], xtab_sem.at[v])

    def early_fwd():
        i, j = origin(ym) * 4 + early_p[0], origin(yp) * 4 + early_p[1]
        col_arrived(i)
        if part_of[0] == "ahead":
            send_col("early_fwd", i, "y+")
        col_arrived(j)
        if part_of[0] == "ahead":
            send_col("early_fwd", j, "y-")

    def early_pass():
        for s in range(2):
            i = origin(y2) * 4 + early_p[s]
            col_arrived(i)
            if part_of[0] == "ahead":
                send_col(("early_pass", s), i, "pair")

    def late_fwd():
        i, j = origin(ym) * 4 + late_p[0], origin(yp) * 4 + late_p[1]
        col_arrived(i)
        send_col("late_fwd", i, "y+")
        col_arrived(j)
        send_col("late_fwd", j, "y-")

    def rows_rest(q):
        row_arrived(x2 * 4 + q, 0)
        row_arrived(x2 * 4 + q, 1)

    def rows_near():
        for q in (pm, pp):
            row_arrived(xm * 4 + q, 1)
            row_arrived(xp * 4 + q, 0)

    def rows_next():
        rows_rest(pm)
        rows_rest(pp)

    def rows_far():
        row_arrived(xm * 4 + p2, 1)
        row_arrived(xp * 4 + p2, 0)

    e0, e1 = early_p
    l0, l1 = late_p

    def products(blocks, wanted, wait=False):
        def product(n, _):
            i = nth(n, [origin(v) * 4 + q for v, q in blocks])
            if wait:
                col_arrived(i)

            @pl.when(wanted(i // 4, i % 4))
            def _():
                block = to_anomaly(rows[i], i)
                column = to_anomaly(cols[i], i)
                for c in range(2):
                    part[c] += lax.dot_general(
                        block, column[c * tile:(c + 1) * tile], contract,
                        preferred_element_type=jnp.float32,
                    )
            return 0

        lax.fori_loop(0, len(blocks), product, 0)

    def now(v, q):
        return (q != p2) & ((q == p) | (v != x2))

    def next_(v, q):
        return (q != p2) & (q != p) & (v == x2)

    def near(v, q):
        return q != p2

    def far(v, q):
        return (q == p2) & (v != x2)

    own_early, own_late = ((y, e0), (y, e1)), ((y, l0), (y, l1))
    side_early, side_early2 = ((ym, e0), (yp, e1)), ((ym, e1), (yp, e0))
    side_late, side_late2 = ((ym, l0), (yp, l1)), ((ym, l1), (yp, l0))
    far_early, far_late = ((y2, e0), (y2, e1)), ((y2, l0), (y2, l1))

    def clear():
        part[...] = jnp.zeros_like(part)
        rows[pl.ds(own, 1)] = x_ref[...][None]

    def a1():
        for q in (e1, e0):
            col_arrived(origin(ym if q is e1 else yp) * 4 + q)
        rows_near()
        products(own_early + side_early + side_early2 + far_early, now)

    def a2():
        rows_next()
        products(own_early + side_early + side_early2 + far_early, next_)
        products(own_late, near)

    def a3():
        products(side_late, near)

    def b1():
        rows_near()
        products(own_late + own_early, now)

    def b2():
        rows_next()
        products(own_late + own_early, next_)
        products(side_late + side_early, near)

    def b3():
        products(side_late2 + side_early2, near, True)

    def b4():
        products(far_early, near)

    def not_last(v, q):
        return (q != p2) | (v != x2)

    def a_far():
        rows_far()
        products(own_early + side_early + side_early2 + far_early + own_late + side_late, far)

    def a_rest():
        products(side_late2 + far_late, not_last, True)

    def b_far():
        rows_far()
        products(own_early + side_early + side_early2 + far_early + own_late + side_late + side_late2, far)

    def b_rest():
        products(far_late, not_last, True)

    def last():
        i = x2 * 4 + p2
        column = to_anomaly(cols[i], i)
        tiles = column[:tile], column[tile:]
        theirs = jnp.where(core == 0, tiles[1], tiles[0])
        mine = jnp.where(core == 0, tiles[0], tiles[1])

        def halves(s):
            return pl.ds(s * half, half)

        def term(s, right):
            block = to_anomaly(rows[i, s * half:(s + 1) * half], i)
            return lax.dot_general(block, right, contract, preferred_element_type=jnp.float32)

        for s in range(2):
            row_arrived(i, s)
            part[1 - core, halves(s)] += term(s, theirs)
        for s in range(2):
            send_small(part.at[1 - core, halves(s)], peer.at[halves(s)], peer_sem.at[s], twin)
            part[core, halves(s)] += term(s, mine)
        for s in range(2):
            arrived(peer.at[halves(s)], peer_sem.at[s])
            out_ref[halves(s)] = (part[core, halves(s)] + peer[halves(s)]) * (1.0 / (MEMBERS - 1))

    def drain_first():
        all_left(FIRST, started["all", FIRST])
        for copy in small[:10]:
            copy.wait_send()

        @pl.when(diagonal)
        def _():
            all_left(PUSH, len(pushes))

        for s, n in turns:
            @pl.when(moves[s])
            def _():
                copy_to(passing.at[s], passing.at[s], pass_sem.at[0], twin, n).wait_send()

    def drain_second():
        all_left(SECOND, started[part_of[0], SECOND])

    def run(steps):
        for step in steps:
            step()

    run((start, pair_sums, means, clear, x_fwd0, near_push, near_push2, z_first, far_rows, turn0, turn1, tables, z_second, x_fwd1a,))

    @pl.when(ahead)
    def _():
        part_of[0] = "ahead"
        run((early0, early1, z_fwd, x_fwd1b, early_fwd, early_pass, tables2, a1, z_far_rows, late0, late1, x_fwd2, drain_first, a2, late_fwd, a3, a_far, drain_second, a_rest,))

    @pl.when(behind)
    def _():
        part_of[0] = "behind"
        run((z_fwd, x_fwd1b, early0, late0, late1, early1, z_far_rows, late_fwd, tables2, b1, x_fwd2, drain_first, early_fwd, b2, b3, early_pass, b4, b_far, drain_second, b_rest,))

    part_of[0] = "all"
    run((last,))

    for copy in small[10:]:
        copy.wait_send()

    @pl.when(ahead)
    def _():
        all_left(THIRD, started["ahead", THIRD])

    @pl.when(behind)
    def _():
        all_left(THIRD, started["behind", THIRD])


def local(snapshots, area_weight):
    members, points = snapshots.shape
    tile = members // 4
    vmem = pl.BlockSpec(memory_space=pltpu.VMEM)
    dma = pltpu.SemaphoreType.DMA
    gram = pl.pallas_call(
        kernel,
        out_shape=jax.ShapeDtypeStruct((members, tile), jnp.float32),
        in_specs=[vmem, vmem],
        out_specs=vmem,
        scratch_shapes=[
            pltpu.VMEM((16, members, points), jnp.bfloat16),
            pltpu.VMEM((16, members // 2, points), jnp.bfloat16),
            pltpu.VMEM((2, members // 2, points), jnp.bfloat16),
            pltpu.VMEM((2, 1, points), jnp.float32),
            pltpu.VMEM((4, 1, points), jnp.float32),
            pltpu.VMEM((16, 2, points), jnp.float32),
            pltpu.VMEM((2, members, tile), jnp.float32),
            pltpu.VMEM((members, tile), jnp.float32),
            dma((16, 2)),
            dma((16,)),
            dma((2,)),
            dma,
            dma((4,)),
            dma((4,)),
            dma((4,)),
            dma((2,)),
            dma((SENDS,)),
        ],
        compiler_params=pltpu.CompilerParams(
            collective_id=0, has_side_effects=True, vmem_limit_bytes=24 * 1024 * 1024
        ),
    )(snapshots, area_weight.reshape(1, points))
    return gram.reshape(1, 1, members * tile)


def solution(mesh):
    return jax.shard_map(
        local,
        mesh=mesh,
        in_specs=(P("mrow", "pcol"), P("pcol")),
        out_specs=P("mrow", "pcol", None),
        check_vma=False,
    )
```

```python
import jax
import jax.numpy as jnp
from jax import lax
from jax.experimental import pallas as pl
from jax.experimental.pallas import tpu as pltpu
from jax.sharding import PartitionSpec as P

MEMBERS = 7424
MESH = pl.DeviceIdType.MESH
SENDS = 18


def device(x, y, p, lo, core):
    return (y * 2 + lo, x * 8 + p * 2 + core)


def kernel(
    x_ref, w_ref, out_ref, rows, cols, passing, sums, ysums, table, part, peer,
    row_sem, col_sem, pass_sem, sum_sem, ysum_sem, ztab_sem, xtab_sem, peer_sem, send_sem,
):
    half = rows.shape[1] // 2
    tile = half // 2
    me_row, me_col = lax.axis_index("mrow"), lax.axis_index("pcol")
    y, lo = me_row // 2, me_row % 2
    x, p, core = me_col // 8, (me_col // 2) % 4, me_col % 2
    hi = p // 2

    xp, xm, x2 = (x + 1) % 4, (x + 3) % 4, (x + 2) % 4
    pp, pm, p2 = (p + 1) % 4, (p + 3) % 4, (p + 2) % 4
    yp, ym, y2 = (y + 1) % 4, (y + 3) % 4, (y + 2) % 4
    x_plus, x_minus, x_far = (device(v, y, p, lo, core) for v in (xp, xm, x2))
    z_plus, z_minus, z_far = (device(x, y, v, lo, core) for v in (pp, pm, p2))
    y_plus, y_minus, y_far = (device(x, v, p, lo, core) for v in (yp, ym, y2))
    z_pair = device(x, y, p, 1 - lo, core)
    twin = device(x, y, p, lo, 1 - core)
    own = x * 4 + p
    diagonal = x == y

    def origin(v):
        return (v + 2 * ((x + v + 1) % 2)) % 4


    turn_lo = [((lo + s - p) % 4) // 2 for s in range(2)]
    turned = [device(x, y, 2 * lo + s, turn_lo[s], core) for s in range(2)]
    stays = [2 * lo + s == p for s in range(2)]
    moves = [jnp.logical_not(v) for v in stays]
    first_p = [(p - hi - 3 * lo) % 4, (p - hi - 1 - lo) % 4]
    second_p = [(p - hi - 3 * (1 - lo)) % 4, (p - hi - 2 + lo) % 4]
    turn_from = [device(x, y, q, hi, core) for q in first_p]
    from_here = [(q == p) & (hi == lo) for q in first_p]
    ahead, behind = hi == lo, hi != lo
    early_p = [jnp.where(ahead, a, b) for a, b in zip(first_p, second_p)]
    late_p = [jnp.where(ahead, b, a) for a, b in zip(first_p, second_p)]

    barrier = pltpu.get_barrier_semaphore()

    def greet(dev):
        pl.semaphore_signal(barrier, inc=1, device_id=dev, device_id_type=MESH)

    for dev in (x_plus, x_minus, x_far, z_plus, z_minus, z_far, y_plus, y_minus, y_far, z_pair, twin):
        greet(dev)
    for s in range(2):
        @pl.when(jnp.logical_not(from_here[s]))
        def _():
            greet(turn_from[s])

    sums[pl.ds(0, 1)] = jnp.sum(x_ref[...].astype(jnp.float32), axis=0, keepdims=True)[None]
    pl.semaphore_wait(barrier, 13 - jnp.where(hi == lo, 1, 0))

    FIRST, SECOND, THIRD, PUSH, TURN, SMALL = 0, 1, 2, 3, 4, 6
    started = {}
    part_of = ["all"]

    def copy_to(src, dst, recv_sem, dev, n):
        return pltpu.make_async_remote_copy(
            src_ref=src, dst_ref=dst, send_sem=send_sem.at[n], recv_sem=recv_sem,
            device_id=dev, device_id_type=MESH,
        )

    def send(name, src, dst, recv_sem, dev):
        if part_of[0] == "all":
            n = FIRST
        elif name[0] in ("far", "fwd2", ("late", 0), ("late", 1), "late_fwd"):
            n = THIRD
        else:
            n = SECOND
        copy_to(src, dst, recv_sem, dev, n).start()
        started[part_of[0], n] = started.get((part_of[0], n), 0) + 1

    def all_left(n, halves):
        blocks = rows.at[pl.ds(0, halves // 2)]
        copy_to(blocks, blocks, pass_sem.at[0], twin, n).wait_send()

    small = []

    def send_small(src, dst, recv_sem, dev):
        copy = copy_to(src, dst, recv_sem, dev, SMALL + len(small))
        copy.start()
        small.append(copy)

    def arrived(ref, recv_sem):
        copy_to(ref, ref, recv_sem, twin, 0).wait_recv()

    def row_half(i, s):
        return rows.at[i, pl.ds(s * half, half)]

    def send_row(name, i, s, way):
        dev = {"x+": x_plus, "x-": x_minus, "z+": z_plus, "z-": z_minus}[way]
        send((name, s, way), row_half(i, s), row_half(i, s), row_sem.at[i, s], dev)

    def row_arrived(i, s):
        arrived(row_half(i, s), row_sem.at[i, s])

    def own_half(s):
        return x_ref.at[pl.ds(s * half, half)]

    def send_own(s, way):
        dev = {"x+": x_plus, "x-": x_minus, "z+": z_plus, "z-": z_minus}[way]
        send(("own", s, way), own_half(s), row_half(own, s), row_sem.at[own, s], dev)

    def send_col(name, i, way):
        dev = {"y+": y_plus, "y-": y_minus, "pair": z_pair}[way]
        send((name, way), cols.at[i], cols.at[i], col_sem.at[i], dev)

    def col_arrived(i):
        arrived(cols.at[i], col_sem.at[i])

    def x_forward(name, q, r):
        i, j = xm * 4 + q, xp * 4 + r
        row_arrived(i, 0)
        send_row(name, i, 0, "x+")
        row_arrived(j, 1)
        send_row(name, j, 1, "x-")

    pushes = []

    def push(src, i, s, dev):
        n = PUSH

        @pl.when(diagonal & stays[s])
        def _():
            copy_to(src, cols.at[i], col_sem.at[i], dev, n).start()

        @pl.when(diagonal & moves[s])
        def _():
            copy_to(src, passing.at[s], pass_sem.at[s], dev, n).start()

        pushes.append((src, n))

    def push_row(v, s, dev):
        push(row_half(v * 4 + p, s), v * 4 + p, s, dev)

    turns = []

    def turn_on(s):
        n = TURN + s
        i = origin(y) * 4 + p

        @pl.when(diagonal & moves[s])
        def _():
            copy_to(row_half(x2 * 4 + p, s), cols.at[i], col_sem.at[i], turned[s], n).start()

        @pl.when(diagonal & stays[s])
        def _():
            cols[pl.ds(i, 1)] = rows[pl.ds(x2 * 4 + p, 1), s * half:(s + 1) * half]

        @pl.when(jnp.logical_not(diagonal) & moves[s])
        def _():
            arrived(passing.at[s], pass_sem.at[s])
            copy_to(passing.at[s], cols.at[i], col_sem.at[i], turned[s], n).start()

        turns.append((s, n))

    def to_anomaly(block, i):
        entry = table[i]
        return ((block.astype(jnp.float32) - entry[0:1]) * entry[1:2]).astype(jnp.bfloat16)

    contract = (((1,), (1,)), ((), ()))

    def nth(n, values):
        value = values[0]
        for k in range(1, len(values)):
            value = jnp.where(n == k, values[k], value)
        return value

    def start():
        send_small(sums.at[0], sums.at[1], sum_sem, z_pair)
        send_own(0, "x+")
        send_own(1, "x-")
        send_own(0, "z+")
        send_own(1, "z-")
        send_own(1, "x+")
        send_own(0, "x-")

    def pair_sums():
        arrived(sums.at[1], sum_sem)
        ysums[pl.ds(y, 1)] = (sums[0] + sums[1])[None]
        for dev in (y_plus, y_minus, y_far):
            send_small(ysums.at[y], ysums.at[y], ysum_sem.at[y], dev)
        push(own_half(0), own, 0, y_far)
        push(own_half(1), own, 1, y_far)

    def means():
        for v in (yp, ym, y2):
            arrived(ysums.at[v], ysum_sem.at[v])
        mean = jnp.sum(ysums[...], axis=0) / MEMBERS
        table[pl.ds(own, 1)] = jnp.concatenate([mean, jnp.sqrt(w_ref[...])], axis=0)[None]
        for dev in (z_plus, z_minus, z_far):
            send_small(table.at[own], table.at[own], ztab_sem.at[p], dev)
        send_own(1, "z+")
        send_own(0, "z-")

    def x_fwd0():
        x_forward("fwd0", p, p)

    def near_push():
        push_row(xm, 0, y_minus)
        push_row(xp, 1, y_plus)

    def z_first():
        i, j = x * 4 + pm, x * 4 + pp
        row_arrived(i, 0)
        send_row("minus", i, 0, "x+")
        row_arrived(j, 1)
        send_row("plus", j, 1, "x-")
        send_row("plus", j, 1, "x+")
        send_row("minus", i, 0, "x-")

    def z_fwd():
        send_row("minus", x * 4 + pm, 0, "z+")
        send_row("plus", x * 4 + pp, 1, "z-")

    def near_push2():
        row_arrived(xm * 4 + p, 1)
        push_row(xm, 1, y_minus)
        row_arrived(xp * 4 + p, 0)
        push_row(xp, 0, y_plus)

    def tables():
        for q in (pp, pm, p2):
            arrived(table.at[x * 4 + q], ztab_sem.at[q])
        group = table.at[pl.ds(x * 4, 4)]
        for dev in (x_plus, x_minus, x_far):
            send_small(group, group, xtab_sem.at[x], dev)

    def far_rows():
        row_arrived(x2 * 4 + p, 0)
        row_arrived(x2 * 4 + p, 1)

    def z_second():
        i, j = x * 4 + pm, x * 4 + pp
        row_arrived(j, 0)
        send_row("plus", j, 0, "x+")
        row_arrived(i, 1)
        send_row("minus", i, 1, "x-")
        send_row("minus", i, 1, "x+")
        send_row("plus", j, 0, "x-")

    def turn0():
        turn_on(0)

    def turn1():
        turn_on(1)

    def x_fwd1a():
        x_forward("fwd1a", pm, pp)

    def x_fwd1b():
        x_forward("fwd1b", pp, pm)

    def x_fwd2():
        x_forward("fwd2", p2, p2)

    def early(s):
        i = origin(y) * 4 + early_p[s]

        @pl.when(jnp.logical_not(from_here[s] & diagonal))
        def _():
            col_arrived(i)

        if part_of[0] == "ahead":
            send_col(("early", s), i, "pair")
        send_col(("early", s), i, "y+")
        send_col(("early", s), i, "y-")

    def late(s):
        i = origin(y) * 4 + late_p[s]
        col_arrived(i)
        if part_of[0] == "behind":
            send_col(("late", s), i, "pair")
        send_col(("late", s), i, "y+")
        send_col(("late", s), i, "y-")

    def early0():
        early(0)

    def early1():
        early(1)

    def late0():
        late(0)

    def late1():
        late(1)

    def z_far_rows():
        k = x * 4 + p2
        row_arrived(k, 0)
        send_row("far", k, 0, "x+")
        row_arrived(k, 1)
        send_row("far", k, 1, "x-")
        send_row("far", k, 1, "x+")
        send_row("far", k, 0, "x-")

    def tables2():
        for v in (xp, xm, x2):
            arrived(table.at[pl.ds(v * 4, 4)], xtab_sem.at[v])

    def early_fwd():
        i, j = origin(ym) * 4 + early_p[0], origin(yp) * 4 + early_p[1]
        col_arrived(i)
        if part_of[0] == "ahead":
            send_col("early_fwd", i, "y+")
        col_arrived(j)
        if part_of[0] == "ahead":
            send_col("early_fwd", j, "y-")

    def early_pass():
        for s in range(2):
            i = origin(y2) * 4 + early_p[s]
            col_arrived(i)
            if part_of[0] == "ahead":
                send_col(("early_pass", s), i, "pair")

    def late_fwd():
        i, j = origin(ym) * 4 + late_p[0], origin(yp) * 4 + late_p[1]
        col_arrived(i)
        send_col("late_fwd", i, "y+")
        col_arrived(j)
        send_col("late_fwd", j, "y-")

    def rows_rest(q):
        row_arrived(x2 * 4 + q, 0)
        row_arrived(x2 * 4 + q, 1)

    def rows_near():
        for q in (pm, pp):
            row_arrived(xm * 4 + q, 1)
            row_arrived(xp * 4 + q, 0)

    def rows_next():
        rows_rest(pm)
        rows_rest(pp)

    def rows_far():
        row_arrived(xm * 4 + p2, 1)
        row_arrived(xp * 4 + p2, 0)

    e0, e1 = early_p
    l0, l1 = late_p

    def products(blocks, wanted, wait=False):
        def product(n, _):
            i = nth(n, [origin(v) * 4 + q for v, q in blocks])
            if wait:
                col_arrived(i)

            @pl.when(wanted(i // 4, i % 4))
            def _():
                block = to_anomaly(rows[i], i)
                column = to_anomaly(cols[i], i)
                for c in range(2):
                    part[c] += lax.dot_general(
                        block, column[c * tile:(c + 1) * tile], contract,
                        preferred_element_type=jnp.float32,
                    )
            return 0

        lax.fori_loop(0, len(blocks), product, 0)

    def now(v, q):
        return (q != p2) & ((q == p) | (v != x2))

    def next_(v, q):
        return (q != p2) & (q != p) & (v == x2)

    def near(v, q):
        return q != p2

    def far(v, q):
        return (q == p2) & (v != x2)

    own_early, own_late = ((y, e0), (y, e1)), ((y, l0), (y, l1))
    side_early, side_early2 = ((ym, e0), (yp, e1)), ((ym, e1), (yp, e0))
    side_late, side_late2 = ((ym, l0), (yp, l1)), ((ym, l1), (yp, l0))
    far_early, far_late = ((y2, e0), (y2, e1)), ((y2, l0), (y2, l1))

    def clear():
        part[...] = jnp.zeros_like(part)
        rows[pl.ds(own, 1)] = x_ref[...][None]

    def a1():
        for q in (e1, e0):
            col_arrived(origin(ym if q is e1 else yp) * 4 + q)
        rows_near()
        products(own_early + side_early + side_early2 + far_early, now)

    def a2():
        rows_next()
        products(own_early + side_early + side_early2 + far_early, next_)
        products(own_late, near)

    def a3():
        products(side_late, near)

    def b1():
        rows_near()
        products(own_late + own_early, now)

    def b2():
        rows_next()
        products(own_late + own_early, next_)
        products(side_late + side_early, near)

    def b3():
        products(side_late2 + side_early2, near, True)

    def b4():
        products(far_early, near)

    def not_last(v, q):
        return (q != p2) | (v != x2)

    def a_far():
        rows_far()
        products(own_early + side_early + side_early2 + far_early + own_late + side_late, far)

    def a_rest():
        products(side_late2 + far_late, not_last, True)

    def b_far():
        rows_far()
        products(own_early + side_early + side_early2 + far_early + own_late + side_late + side_late2, far)

    def b_rest():
        products(far_late, not_last, True)

    def last():
        i = x2 * 4 + p2
        column = to_anomaly(cols[i], i)
        tiles = column[:tile], column[tile:]
        theirs = jnp.where(core == 0, tiles[1], tiles[0])
        mine = jnp.where(core == 0, tiles[0], tiles[1])

        def halves(s):
            return pl.ds(s * half, half)

        def term(s, right):
            block = to_anomaly(rows[i, s * half:(s + 1) * half], i)
            return lax.dot_general(block, right, contract, preferred_element_type=jnp.float32)

        for s in range(2):
            row_arrived(i, s)
            part[1 - core, halves(s)] += term(s, theirs)
        for s in range(2):
            send_small(part.at[1 - core, halves(s)], peer.at[halves(s)], peer_sem.at[s], twin)
            part[core, halves(s)] += term(s, mine)
        for s in range(2):
            arrived(peer.at[halves(s)], peer_sem.at[s])
            out_ref[halves(s)] = (part[core, halves(s)] + peer[halves(s)]) * (1.0 / (MEMBERS - 1))

    def drain_first():
        all_left(FIRST, started["all", FIRST])
        for copy in small[:10]:
            copy.wait_send()

        @pl.when(diagonal)
        def _():
            all_left(PUSH, len(pushes))

        for s, n in turns:
            @pl.when(moves[s])
            def _():
                copy_to(passing.at[s], passing.at[s], pass_sem.at[0], twin, n).wait_send()

    def drain_second():
        all_left(SECOND, started[part_of[0], SECOND])

    def run(steps):
        for step in steps:
            step()

    run((start, pair_sums, means, clear, x_fwd0, near_push, near_push2, z_first, far_rows, turn1, turn0, tables, z_second, x_fwd1a,))

    @pl.when(ahead)
    def _():
        part_of[0] = "ahead"
        run((early0, early1, z_fwd, x_fwd1b, early_fwd, early_pass, tables2, a1, z_far_rows, late0, late1, x_fwd2, drain_first, a2, late_fwd, a3, a_far, drain_second, a_rest,))

    @pl.when(behind)
    def _():
        part_of[0] = "behind"
        run((z_fwd, x_fwd1b, early0, late0, late1, early1, z_far_rows, late_fwd, tables2, b1, x_fwd2, drain_first, early_fwd, b2, b3, early_pass, b4, b_far, drain_second, b_rest,))

    part_of[0] = "all"
    run((last,))

    for copy in small[10:]:
        copy.wait_send()

    @pl.when(ahead)
    def _():
        all_left(THIRD, started["ahead", THIRD])

    @pl.when(behind)
    def _():
        all_left(THIRD, started["behind", THIRD])


def local(snapshots, area_weight):
    members, points = snapshots.shape
    tile = members // 4
    vmem = pl.BlockSpec(memory_space=pltpu.VMEM)
    dma = pltpu.SemaphoreType.DMA
    gram = pl.pallas_call(
        kernel,
        out_shape=jax.ShapeDtypeStruct((members, tile), jnp.float32),
        in_specs=[vmem, vmem],
        out_specs=vmem,
        scratch_shapes=[
            pltpu.VMEM((16, members, points), jnp.bfloat16),
            pltpu.VMEM((16, members // 2, points), jnp.bfloat16),
            pltpu.VMEM((2, members // 2, points), jnp.bfloat16),
            pltpu.VMEM((2, 1, points), jnp.float32),
            pltpu.VMEM((4, 1, points), jnp.float32),
            pltpu.VMEM((16, 2, points), jnp.float32),
            pltpu.VMEM((2, members, tile), jnp.float32),
            pltpu.VMEM((members, tile), jnp.float32),
            dma((16, 2)),
            dma((16,)),
            dma((2,)),
            dma,
            dma((4,)),
            dma((4,)),
            dma((4,)),
            dma((2,)),
            dma((SENDS,)),
        ],
        compiler_params=pltpu.CompilerParams(
            collective_id=0, has_side_effects=True, vmem_limit_bytes=24 * 1024 * 1024
        ),
    )(snapshots, area_weight.reshape(1, points))
    return gram.reshape(1, 1, members * tile)


def solution(mesh):
    return jax.shard_map(
        local,
        mesh=mesh,
        in_specs=(P("mrow", "pcol"), P("pcol")),
        out_specs=P("mrow", "pcol", None),
        check_vma=False,
    )
```

```python
import jax
import jax.numpy as jnp
from jax import lax
from jax.experimental import pallas as pl
from jax.experimental.pallas import tpu as pltpu
from jax.sharding import PartitionSpec as P

MEMBERS = 7424
MESH = pl.DeviceIdType.MESH
SENDS = 18


def device(x, y, p, lo, core):
    return (y * 2 + lo, x * 8 + p * 2 + core)


def kernel(
    x_ref, w_ref, out_ref, rows, cols, passing, sums, ysums, table, part, peer,
    row_sem, col_sem, pass_sem, sum_sem, ysum_sem, ztab_sem, xtab_sem, peer_sem, send_sem,
):
    half = rows.shape[1] // 2
    tile = half // 2
    me_row, me_col = lax.axis_index("mrow"), lax.axis_index("pcol")
    y, lo = me_row // 2, me_row % 2
    x, p, core = me_col // 8, (me_col // 2) % 4, me_col % 2
    hi = p // 2

    xp, xm, x2 = (x + 1) % 4, (x + 3) % 4, (x + 2) % 4
    pp, pm, p2 = (p + 1) % 4, (p + 3) % 4, (p + 2) % 4
    yp, ym, y2 = (y + 1) % 4, (y + 3) % 4, (y + 2) % 4
    x_plus, x_minus, x_far = (device(v, y, p, lo, core) for v in (xp, xm, x2))
    z_plus, z_minus, z_far = (device(x, y, v, lo, core) for v in (pp, pm, p2))
    y_plus, y_minus, y_far = (device(x, v, p, lo, core) for v in (yp, ym, y2))
    z_pair = device(x, y, p, 1 - lo, core)
    twin = device(x, y, p, lo, 1 - core)
    own = x * 4 + p
    diagonal = x == y

    def origin(v):
        return (v + 2 * ((x + v + 1) % 2)) % 4


    turn_lo = [((lo + s - p) % 4) // 2 for s in range(2)]
    turned = [device(x, y, 2 * lo + s, turn_lo[s], core) for s in range(2)]
    stays = [2 * lo + s == p for s in range(2)]
    moves = [jnp.logical_not(v) for v in stays]
    first_p = [(p - hi - 3 * lo) % 4, (p - hi - 1 - lo) % 4]
    second_p = [(p - hi - 3 * (1 - lo)) % 4, (p - hi - 2 + lo) % 4]
    turn_from = [device(x, y, q, hi, core) for q in first_p]
    from_here = [(q == p) & (hi == lo) for q in first_p]
    ahead, behind = hi == lo, hi != lo
    early_p = [jnp.where(ahead, a, b) for a, b in zip(first_p, second_p)]
    late_p = [jnp.where(ahead, b, a) for a, b in zip(first_p, second_p)]

    barrier = pltpu.get_barrier_semaphore()

    def greet(dev):
        pl.semaphore_signal(barrier, inc=1, device_id=dev, device_id_type=MESH)

    for dev in (x_plus, x_minus, x_far, z_plus, z_minus, z_far, y_plus, y_minus, y_far, z_pair, twin):
        greet(dev)
    for s in range(2):
        @pl.when(jnp.logical_not(from_here[s]))
        def _():
            greet(turn_from[s])

    sums[pl.ds(0, 1)] = jnp.sum(x_ref[...].astype(jnp.float32), axis=0, keepdims=True)[None]
    pl.semaphore_wait(barrier, 13 - jnp.where(hi == lo, 1, 0))

    FIRST, SECOND, THIRD, PUSH, TURN, SMALL = 0, 1, 2, 3, 4, 6
    started = {}
    part_of = ["all"]

    def copy_to(src, dst, recv_sem, dev, n):
        return pltpu.make_async_remote_copy(
            src_ref=src, dst_ref=dst, send_sem=send_sem.at[n], recv_sem=recv_sem,
            device_id=dev, device_id_type=MESH,
        )

    def send(name, src, dst, recv_sem, dev):
        if part_of[0] == "all":
            n = FIRST
        elif name[0] in ("far", "fwd2", ("late", 0), ("late", 1), "late_fwd"):
            n = THIRD
        else:
            n = SECOND
        copy_to(src, dst, recv_sem, dev, n).start()
        started[part_of[0], n] = started.get((part_of[0], n), 0) + 1

    def all_left(n, halves):
        blocks = rows.at[pl.ds(0, halves // 2)]
        copy_to(blocks, blocks, pass_sem.at[0], twin, n).wait_send()

    small = []

    def send_small(src, dst, recv_sem, dev):
        copy = copy_to(src, dst, recv_sem, dev, SMALL + len(small))
        copy.start()
        small.append(copy)

    def arrived(ref, recv_sem):
        copy_to(ref, ref, recv_sem, twin, 0).wait_recv()

    def row_half(i, s):
        return rows.at[i, pl.ds(s * half, half)]

    def send_row(name, i, s, way):
        dev = {"x+": x_plus, "x-": x_minus, "z+": z_plus, "z-": z_minus}[way]
        send((name, s, way), row_half(i, s), row_half(i, s), row_sem.at[i, s], dev)

    def row_arrived(i, s):
        arrived(row_half(i, s), row_sem.at[i, s])

    def own_half(s):
        return x_ref.at[pl.ds(s * half, half)]

    def send_own(s, way):
        dev = {"x+": x_plus, "x-": x_minus, "z+": z_plus, "z-": z_minus}[way]
        send(("own", s, way), own_half(s), row_half(own, s), row_sem.at[own, s], dev)

    def send_col(name, i, way):
        dev = {"y+": y_plus, "y-": y_minus, "pair": z_pair}[way]
        send((name, way), cols.at[i], cols.at[i], col_sem.at[i], dev)

    def col_arrived(i):
        arrived(cols.at[i], col_sem.at[i])

    def x_forward(name, q, r):
        i, j = xm * 4 + q, xp * 4 + r
        row_arrived(i, 0)
        send_row(name, i, 0, "x+")
        row_arrived(j, 1)
        send_row(name, j, 1, "x-")

    pushes = []

    def push(src, i, s, dev):
        n = PUSH

        @pl.when(diagonal & stays[s])
        def _():
            copy_to(src, cols.at[i], col_sem.at[i], dev, n).start()

        @pl.when(diagonal & moves[s])
        def _():
            copy_to(src, passing.at[s], pass_sem.at[s], dev, n).start()

        pushes.append((src, n))

    def push_row(v, s, dev):
        push(row_half(v * 4 + p, s), v * 4 + p, s, dev)

    turns = []

    def turn_on(s):
        n = TURN + s
        i = origin(y) * 4 + p

        @pl.when(diagonal & moves[s])
        def _():
            copy_to(row_half(x2 * 4 + p, s), cols.at[i], col_sem.at[i], turned[s], n).start()

        @pl.when(diagonal & stays[s])
        def _():
            cols[pl.ds(i, 1)] = rows[pl.ds(x2 * 4 + p, 1), s * half:(s + 1) * half]

        @pl.when(jnp.logical_not(diagonal) & moves[s])
        def _():
            arrived(passing.at[s], pass_sem.at[s])
            copy_to(passing.at[s], cols.at[i], col_sem.at[i], turned[s], n).start()

        turns.append((s, n))

    def to_anomaly(block, i):
        entry = table[i]
        return ((block.astype(jnp.float32) - entry[0:1]) * entry[1:2]).astype(jnp.bfloat16)

    contract = (((1,), (1,)), ((), ()))

    def nth(n, values):
        value = values[0]
        for k in range(1, len(values)):
            value = jnp.where(n == k, values[k], value)
        return value

    def start():
        send_small(sums.at[0], sums.at[1], sum_sem, z_pair)
        send_own(0, "x+")
        send_own(1, "x-")
        send_own(0, "z+")
        send_own(1, "z-")
        send_own(1, "x+")
        send_own(0, "x-")

    def pair_sums():
        arrived(sums.at[1], sum_sem)
        ysums[pl.ds(y, 1)] = (sums[0] + sums[1])[None]
        for dev in (y_plus, y_minus, y_far):
            send_small(ysums.at[y], ysums.at[y], ysum_sem.at[y], dev)
        push(own_half(0), own, 0, y_far)
        push(own_half(1), own, 1, y_far)

    def means():
        for v in (yp, ym, y2):
            arrived(ysums.at[v], ysum_sem.at[v])
        mean = jnp.sum(ysums[...], axis=0) / MEMBERS
        table[pl.ds(own, 1)] = jnp.concatenate([mean, jnp.sqrt(w_ref[...])], axis=0)[None]
        for dev in (z_plus, z_minus, z_far):
            send_small(table.at[own], table.at[own], ztab_sem.at[p], dev)
        send_own(1, "z+")
        send_own(0, "z-")

    def x_fwd0():
        x_forward("fwd0", p, p)

    def near_push():
        push_row(xm, 0, y_minus)
        push_row(xp, 1, y_plus)

    def z_first():
        i, j = x * 4 + pm, x * 4 + pp
        row_arrived(i, 0)
        send_row("minus", i, 0, "x+")
        row_arrived(j, 1)
        send_row("plus", j, 1, "x-")
        send_row("plus", j, 1, "x+")
        send_row("minus", i, 0, "x-")

    def z_fwd():
        send_row("minus", x * 4 + pm, 0, "z+")
        send_row("plus", x * 4 + pp, 1, "z-")

    def near_push2():
        row_arrived(xm * 4 + p, 1)
        push_row(xm, 1, y_minus)
        row_arrived(xp * 4 + p, 0)
        push_row(xp, 0, y_plus)

    def tables():
        for q in (pp, pm, p2):
            arrived(table.at[x * 4 + q], ztab_sem.at[q])
        group = table.at[pl.ds(x * 4, 4)]
        for dev in (x_plus, x_minus, x_far):
            send_small(group, group, xtab_sem.at[x], dev)

    def far_rows():
        row_arrived(x2 * 4 + p, 0)
        row_arrived(x2 * 4 + p, 1)

    def z_second():
        i, j = x * 4 + pm, x * 4 + pp
        row_arrived(j, 0)
        send_row("plus", j, 0, "x+")
        row_arrived(i, 1)
        send_row("minus", i, 1, "x-")
        send_row("minus", i, 1, "x+")
        send_row("plus", j, 0, "x-")

    def turn0():
        turn_on(0)

    def turn1():
        turn_on(1)

    def x_fwd1a():
        x_forward("fwd1a", pm, pp)

    def x_fwd1b():
        x_forward("fwd1b", pp, pm)

    def x_fwd2():
        x_forward("fwd2", p2, p2)

    def early(s):
        i = origin(y) * 4 + early_p[s]

        @pl.when(jnp.logical_not(from_here[s] & diagonal))
        def _():
            col_arrived(i)

        if part_of[0] == "ahead":
            send_col(("early", s), i, "pair")
        send_col(("early", s), i, "y+")
        send_col(("early", s), i, "y-")

    def late(s):
        i = origin(y) * 4 + late_p[s]
        col_arrived(i)
        if part_of[0] == "behind":
            send_col(("late", s), i, "pair")
        send_col(("late", s), i, "y+")
        send_col(("late", s), i, "y-")

    def early0():
        early(0)

    def early1():
        early(1)

    def late0():
        late(0)

    def late1():
        late(1)

    def z_far_rows():
        k = x * 4 + p2
        row_arrived(k, 0)
        send_row("far", k, 0, "x+")
        row_arrived(k, 1)
        send_row("far", k, 1, "x-")
        send_row("far", k, 1, "x+")
        send_row("far", k, 0, "x-")

    def tables2():
        for v in (xp, xm, x2):
            arrived(table.at[pl.ds(v * 4, 4)], xtab_sem.at[v])

    def early_fwd():
        i, j = origin(ym) * 4 + early_p[0], origin(yp) * 4 + early_p[1]
        col_arrived(i)
        if part_of[0] == "ahead":
            send_col("early_fwd", i, "y+")
        col_arrived(j)
        if part_of[0] == "ahead":
            send_col("early_fwd", j, "y-")

    def early_pass():
        for s in range(2):
            i = origin(y2) * 4 + early_p[s]
            col_arrived(i)
            if part_of[0] == "ahead":
                send_col(("early_pass", s), i, "pair")

    def late_fwd():
        i, j = origin(ym) * 4 + late_p[0], origin(yp) * 4 + late_p[1]
        col_arrived(i)
        send_col("late_fwd", i, "y+")
        col_arrived(j)
        send_col("late_fwd", j, "y-")

    def rows_rest(q):
        row_arrived(x2 * 4 + q, 0)
        row_arrived(x2 * 4 + q, 1)

    def rows_near():
        for q in (pm, pp):
            row_arrived(xm * 4 + q, 1)
            row_arrived(xp * 4 + q, 0)

    def rows_next():
        rows_rest(pm)
        rows_rest(pp)

    def rows_far():
        row_arrived(xm * 4 + p2, 1)
        row_arrived(xp * 4 + p2, 0)

    e0, e1 = early_p
    l0, l1 = late_p

    def products(blocks, wanted, wait=False):
        def product(n, _):
            i = nth(n, [origin(v) * 4 + q for v, q in blocks])
            if wait:
                col_arrived(i)

            @pl.when(wanted(i // 4, i % 4))
            def _():
                block = to_anomaly(rows[i], i)
                column = to_anomaly(cols[i], i)
                for c in range(2):
                    part[c] += lax.dot_general(
                        block, column[c * tile:(c + 1) * tile], contract,
                        preferred_element_type=jnp.float32,
                    )
            return 0

        lax.fori_loop(0, len(blocks), product, 0)

    def now(v, q):
        return (q != p2) & ((q == p) | (v != x2))

    def next_(v, q):
        return (q != p2) & (q != p) & (v == x2)

    def near(v, q):
        return q != p2

    def far(v, q):
        return (q == p2) & (v != x2)

    own_early, own_late = ((y, e0), (y, e1)), ((y, l0), (y, l1))
    side_early, side_early2 = ((ym, e0), (yp, e1)), ((ym, e1), (yp, e0))
    side_late, side_late2 = ((ym, l0), (yp, l1)), ((ym, l1), (yp, l0))
    far_early, far_late = ((y2, e0), (y2, e1)), ((y2, l0), (y2, l1))

    def clear():
        part[...] = jnp.zeros_like(part)
        rows[pl.ds(own, 1)] = x_ref[...][None]

    def a1():
        for q in (e1, e0):
            col_arrived(origin(ym if q is e1 else yp) * 4 + q)
        rows_near()
        products(own_early + side_early + side_early2 + far_early, now)

    def a2():
        rows_next()
        products(own_early + side_early + side_early2 + far_early, next_)
        products(own_late, near)

    def a3():
        products(side_late, near)

    def b1():
        rows_near()
        products(own_late + own_early, now)

    def b2():
        rows_next()
        products(own_late + own_early, next_)
        products(side_late + side_early, near)

    def b3():
        products(side_late2 + side_early2, near, True)

    def b4():
        products(far_early, near)

    def not_last(v, q):
        return (q != p2) | (v != x2)

    def a_far():
        rows_far()
        products(own_early + side_early + side_early2 + far_early + own_late + side_late, far)

    def a_rest():
        products(side_late2 + far_late, not_last, True)

    def b_far():
        rows_far()
        products(own_early + side_early + side_early2 + far_early + own_late + side_late + side_late2, far)

    def b_rest():
        products(far_late, not_last, True)

    def last():
        i = x2 * 4 + p2
        column = to_anomaly(cols[i], i)
        tiles = column[:tile], column[tile:]
        theirs = jnp.where(core == 0, tiles[1], tiles[0])
        mine = jnp.where(core == 0, tiles[0], tiles[1])

        def halves(s):
            return pl.ds(s * half, half)

        def term(s, right):
            block = to_anomaly(rows[i, s * half:(s + 1) * half], i)
            return lax.dot_general(block, right, contract, preferred_element_type=jnp.float32)

        for s in range(2):
            row_arrived(i, s)
            part[1 - core, halves(s)] += term(s, theirs)
        for s in range(2):
            send_small(part.at[1 - core, halves(s)], peer.at[halves(s)], peer_sem.at[s], twin)
            part[core, halves(s)] += term(s, mine)
        for s in range(2):
            arrived(peer.at[halves(s)], peer_sem.at[s])
            out_ref[halves(s)] = (part[core, halves(s)] + peer[halves(s)]) * (1.0 / (MEMBERS - 1))

    def drain_first():
        all_left(FIRST, started["all", FIRST])
        for copy in small[:10]:
            copy.wait_send()

        @pl.when(diagonal)
        def _():
            all_left(PUSH, len(pushes))

        for s, n in turns:
            @pl.when(moves[s])
            def _():
                copy_to(passing.at[s], passing.at[s], pass_sem.at[0], twin, n).wait_send()

    def drain_second():
        all_left(SECOND, started[part_of[0], SECOND])

    def run(steps):
        for step in steps:
            step()

    run((start, pair_sums, means, clear, x_fwd0, near_push, near_push2, z_first, far_rows, turn1, turn0, tables, z_second, x_fwd1a,))

    @pl.when(ahead)
    def _():
        part_of[0] = "ahead"
        run((early0, early1, z_fwd, x_fwd1b, early_fwd, early_pass, tables2, a1, z_far_rows, late0, late1, x_fwd2, drain_first, late_fwd, a2, a3, a_far, drain_second, a_rest,))

    @pl.when(behind)
    def _():
        part_of[0] = "behind"
        run((z_fwd, x_fwd1b, early0, late0, late1, early1, z_far_rows, late_fwd, tables2, b1, x_fwd2, drain_first, early_fwd, b2, b3, early_pass, b4, b_far, drain_second, b_rest,))

    part_of[0] = "all"
    run((last,))

    for copy in small[10:]:
        copy.wait_send()

    @pl.when(ahead)
    def _():
        all_left(THIRD, started["ahead", THIRD])

    @pl.when(behind)
    def _():
        all_left(THIRD, started["behind", THIRD])


def local(snapshots, area_weight):
    members, points = snapshots.shape
    tile = members // 4
    vmem = pl.BlockSpec(memory_space=pltpu.VMEM)
    dma = pltpu.SemaphoreType.DMA
    gram = pl.pallas_call(
        kernel,
        out_shape=jax.ShapeDtypeStruct((members, tile), jnp.float32),
        in_specs=[vmem, vmem],
        out_specs=vmem,
        scratch_shapes=[
            pltpu.VMEM((16, members, points), jnp.bfloat16),
            pltpu.VMEM((16, members // 2, points), jnp.bfloat16),
            pltpu.VMEM((2, members // 2, points), jnp.bfloat16),
            pltpu.VMEM((2, 1, points), jnp.float32),
            pltpu.VMEM((4, 1, points), jnp.float32),
            pltpu.VMEM((16, 2, points), jnp.float32),
            pltpu.VMEM((2, members, tile), jnp.float32),
            pltpu.VMEM((members, tile), jnp.float32),
            dma((16, 2)),
            dma((16,)),
            dma((2,)),
            dma,
            dma((4,)),
            dma((4,)),
            dma((4,)),
            dma((2,)),
            dma((SENDS,)),
        ],
        compiler_params=pltpu.CompilerParams(
            collective_id=0, has_side_effects=True, vmem_limit_bytes=24 * 1024 * 1024
        ),
    )(snapshots, area_weight.reshape(1, points))
    return gram.reshape(1, 1, members * tile)


def solution(mesh):
    return jax.shard_map(
        local,
        mesh=mesh,
        in_specs=(P("mrow", "pcol"), P("pcol")),
        out_specs=P("mrow", "pcol", None),
        check_vma=False,
    )
```
